8 devices in a mesh: replica: 1 (over z), model: 8 (over y, x, core).
Axes of the slice: x: 2, y: 2, z: 1, core: 2. Of those that a mesh axis runs over, the one named last changes fastest.
Arguments:
- x: bfloat16 [6, 7168], P('replica')
- w_q: bfloat16 [7168, 16384], P(None, 'model')
- w_k: bfloat16 [7168, 256], replicated
- w_v: bfloat16 [7168, 256], replicated
- w_o: bfloat16 [16384, 7168], P('model')
- k_cache: bfloat16 [6, 1, 16384, 256], P('replica', None, 'model')
- v_cache: bfloat16 [6, 1, 16384, 256], P('replica', None, 'model')
- lengths: int32 [6], P('replica')
Outputs:
- output 1: bfloat16 [6, 7168], P('replica')
- output 2: bfloat16 [6, 256], P('replica')
- output 3: bfloat16 [6, 256], P('replica')
All inputs are finite; a program needn't handle non-finite values.
Results may differ from the reference program's by a relative error of at most 0.00765567.
Values are sent between devices in bfloat16 or wider.
A program may use at most 1 GiB of HBM per device.

```python
import jax
import jax.numpy as jnp
from jax import lax

B = 6
T = 16384
D = 7168
HEADS = 64
KV_HEADS = 1
HEAD = 256


def draw_lengths(key):
    keys = jax.random.split(key, 4)
    base = jax.random.randint(keys[0], (B,), 1, T)
    long_slot = jax.random.randint(keys[1], (), 0, B)
    short_slot = (long_slot + 1 + jax.random.randint(keys[2], (), 0, max(B - 1, 1))) % B
    short_len = jax.random.randint(keys[3], (), 1, 9)
    slots = jnp.arange(B)
    lengths = jnp.where(slots == short_slot, short_len, base)
    return jnp.where(slots == long_slot, T - 1, lengths).astype(jnp.int32)


def setup_inputs(seed: int = 0, part: int = 0) -> dict:
    key = jax.random.key(seed)
    shared = jax.random.split(key, 4)
    own = jax.random.split(jax.random.fold_in(key, part), 4)
    in_scale = D ** -0.5
    out_scale = (HEADS * HEAD) ** -0.5
    w_q = (jax.random.normal(shared[0], (D, HEADS * HEAD), jnp.float32) * in_scale).astype(jnp.bfloat16)
    w_k = (jax.random.normal(shared[1], (D, KV_HEADS * HEAD), jnp.float32) * in_scale).astype(jnp.bfloat16)
    w_v = (jax.random.normal(shared[2], (D, KV_HEADS * HEAD), jnp.float32) * in_scale).astype(jnp.bfloat16)
    w_o = (jax.random.normal(shared[3], (HEADS * HEAD, D), jnp.float32) * out_scale).astype(jnp.bfloat16)
    x = jax.random.normal(own[0], (B, D), jnp.float32).astype(jnp.bfloat16)
    lengths = draw_lengths(own[1])
    k_cache = jax.random.normal(own[2], (B, KV_HEADS, T, HEAD), jnp.float32).astype(jnp.bfloat16)
    v_scale = 0.6 * jnp.sqrt(lengths.astype(jnp.float32) + 1.0)
    v_cache = (jax.random.normal(own[3], (B, KV_HEADS, T, HEAD), jnp.float32) * v_scale[:, None, None, None]).astype(jnp.bfloat16)
    return {'x': x, 'w_q': w_q, 'w_k': w_k, 'w_v': w_v, 'w_o': w_o, 'k_cache': k_cache, 'v_cache': v_cache, 'lengths': lengths}


def reference(x, w_q, w_k, w_v, w_o, k_cache, v_cache, lengths):
    group = HEADS // KV_HEADS
    scale = HEAD ** -0.5
    q_all = jnp.dot(x, w_q, preferred_element_type=jnp.float32).astype(jnp.bfloat16)
    k_new = jnp.dot(x, w_k, preferred_element_type=jnp.float32).astype(jnp.bfloat16)
    v_new = jnp.dot(x, w_v, preferred_element_type=jnp.float32).astype(jnp.bfloat16)
    positions = jnp.arange(T)

    def one_sequence(items):
        q_row, k_rows, v_rows, k_last, v_last, seq_len = items
        q_heads = q_row.reshape(KV_HEADS, group, HEAD).astype(jnp.float32)
        scores = jnp.einsum('kgd,ktd->kgt', q_heads, k_rows.astype(jnp.float32)) * scale
        scores = jnp.where(positions < seq_len, scores, -jnp.inf)
        score_new = jnp.einsum('kgd,kd->kg', q_heads, k_last.reshape(KV_HEADS, HEAD).astype(jnp.float32)) * scale
        top = jnp.maximum(jnp.max(scores, axis=-1), score_new)
        weights = jnp.exp(scores - top[:, :, None])
        weight_new = jnp.exp(score_new - top)
        total = jnp.sum(weights, axis=-1) + weight_new
        out = jnp.einsum('kgt,ktd->kgd', weights, v_rows.astype(jnp.float32))
        out = out + weight_new[:, :, None] * v_last.reshape(KV_HEADS, 1, HEAD).astype(jnp.float32)
        return (out / total[:, :, None]).astype(jnp.bfloat16).reshape(HEADS * HEAD)

    attn = lax.map(one_sequence, (q_all, k_cache, v_cache, k_new, v_new, lengths))
    y_out = (x.astype(jnp.float32) + jnp.dot(attn, w_o, preferred_element_type=jnp.float32)).astype(jnp.bfloat16)
    return (y_out, k_new, v_new)
```

```python
import functools
import math

import jax
import jax.numpy as jnp
from jax import lax
from jax.experimental import pallas as pl
from jax.experimental.pallas import tpu as pltpu
from jax.sharding import PartitionSpec as P

RING = 4
LANES = 128


def peer_of(me, k, n_dev):
    return lax.rem(me + k, n_dev)


def kernel(n_dev, x_hbm, wq_hbm, wk_hbm, wv_hbm, wo_hbm, kc_hbm, vc_hbm, len_ref,
           y_out, k_out, v_out,
           x_v, wq_v, wkv_v, k_v, v_v, wo_v,
           qbuf, kvbuf, osend, obuf, mlsend, mlbuf, astage, a_v, ysend, ybuf, y_v, kvout_v,
           x_sem, wq_sem, wkv_sem, k_sem, v_sem, wo_sem, out_sem,
           q_ssem, q_rsem, kv_ssem, kv_rsem, o_ssem, o_rsem, ml_ssem, ml_rsem,
           y_ssem, y_rsem, g_ssem, g_rsem):
    rows, depth = x_hbm.shape
    head_dim = wk_hbm.shape[1]
    own_heads = wq_hbm.shape[1] // head_dim
    t_local = kc_hbm.shape[2]
    heads = own_heads * n_dev
    kv_rows = depth // n_dev
    y_cols = wo_hbm.shape[1] // n_dev
    me = lax.axis_index("model")
    factor = head_dim ** -0.5 * math.log2(math.e)
    f32, bf16 = jnp.float32, jnp.bfloat16

    def head_cols(h):
        return pl.ds(pl.multiple_of(h * head_dim, head_dim), head_dim)

    def own_cols(p):
        return pl.ds(pl.multiple_of(p * y_cols, LANES), y_cols)

    def wq_copy(h):
        slot = lax.rem(h, RING)
        return pltpu.make_async_copy(wq_hbm.at[:, head_cols(h)], wq_v.at[slot], wq_sem.at[slot])

    def wo_copy(j):
        p = lax.rem(me + 1 + j, n_dev)
        return pltpu.make_async_copy(wo_hbm.at[:, own_cols(p)], wo_v.at[j], wo_sem.at[j])

    kv_slice = pl.ds(pl.multiple_of(me * kv_rows, LANES), kv_rows)
    x_copy = pltpu.make_async_copy(x_hbm, x_v, x_sem)
    wk_copy = pltpu.make_async_copy(wk_hbm.at[kv_slice, :], wkv_v.at[0], wkv_sem.at[0])
    wv_copy = pltpu.make_async_copy(wv_hbm.at[kv_slice, :], wkv_v.at[1], wkv_sem.at[1])

    def k_copy(b):
        return pltpu.make_async_copy(kc_hbm.at[b, 0], k_v.at[b], k_sem.at[b])

    def v_copy(b):
        return pltpu.make_async_copy(vc_hbm.at[b, 0], v_v.at[b], v_sem.at[b])

    x_copy.start()
    for h in range(RING):
        wq_copy(h).start()

    barrier = pltpu.get_barrier_semaphore()
    for k in range(1, n_dev):
        pl.semaphore_signal(barrier, inc=1, device_id={"model": peer_of(me, k, n_dev)},
                            device_id_type=pl.DeviceIdType.MESH)
    pl.semaphore_wait(barrier, n_dev - 1)
    x_copy.wait()

    def send_all(src, dst, ssem, rsem):
        def body(k, c):
            pltpu.make_async_remote_copy(
                src_ref=src, dst_ref=dst, send_sem=ssem, recv_sem=rsem,
                device_id={"model": peer_of(me, k, n_dev)},
                device_id_type=pl.DeviceIdType.MESH).start()
            return c
        lax.fori_loop(1, n_dev, body, 0, unroll=True)

    def wait_bytes(ref, sem):
        pltpu.make_async_copy(ref, ref, sem).wait()

    def q_step(h, c):
        wq_copy(h).wait()
        q = jnp.dot(x_v[...], wq_v[lax.rem(h, RING)], preferred_element_type=f32)
        block = me * own_heads + h
        qbuf[block] = q.astype(bf16).astype(f32)
        send_all(qbuf.at[block], qbuf.at[block], q_ssem, q_rsem)

        @pl.when(h < own_heads - RING)
        def _():
            wq_copy(h + RING).start()

        @pl.when(h == own_heads - RING - 1)
        def _():
            wk_copy.start()
            wv_copy.start()
            for b in range(rows):
                k_copy(b).start()
                v_copy(b).start()
            for j in range(n_dev):
                wo_copy(j).start()
        return c

    lax.fori_loop(0, own_heads, q_step, 0)

    wk_copy.wait()
    wv_copy.wait()
    x_part = x_v[:, kv_slice]
    for i in range(2):
        kvbuf[me, i] = jnp.dot(x_part, wkv_v[i], preferred_element_type=f32)
    send_all(kvbuf.at[me], kvbuf.at[me], kv_ssem, kv_rsem)

    wait_bytes(qbuf.at[pl.ds(0, heads - own_heads)], q_rsem)

    positions = me * t_local + lax.broadcasted_iota(jnp.int32, (1, t_local), 1)
    lane = lax.broadcasted_iota(jnp.int32, (heads, LANES), 1)

    def attend(b, ml):
        k_copy(b).wait()
        q_b = qbuf[:, b, :].astype(bf16)
        s = lax.dot_general(q_b, k_v[b], (((1,), (1,)), ((), ())), preferred_element_type=f32)
        s = jnp.where(positions < len_ref[b], s, -jnp.inf)
        m = jnp.max(s, axis=1, keepdims=True)
        m_safe = jnp.where(m == -jnp.inf, 0.0, m)
        p = jnp.exp2((s - m_safe) * factor)
        l = jnp.sum(p, axis=1, keepdims=True)
        hi = p.astype(bf16)
        lo = (p - hi.astype(f32)).astype(bf16)
        v_copy(b).wait()
        o2 = jnp.dot(jnp.concatenate([hi, lo], axis=0), v_v[b], preferred_element_type=f32)
        osend[b] = o2[:heads] + o2[heads:]
        obuf[me, b] = osend[b, pl.ds(pl.multiple_of(me * own_heads, 8), own_heads), :]

        def send(k, c):
            p_dev = peer_of(me, k, n_dev)
            pltpu.make_async_remote_copy(
                src_ref=osend.at[b, pl.ds(pl.multiple_of(p_dev * own_heads, 8), own_heads), :],
                dst_ref=obuf.at[me, b], send_sem=o_ssem, recv_sem=o_rsem,
                device_id={"model": p_dev}, device_id_type=pl.DeviceIdType.MESH).start()
            return c
        lax.fori_loop(1, n_dev, send, 0, unroll=True)
        ml = jnp.where(lane == b, m, ml)
        return jnp.where(lane == b + 8, l, ml)

    ml = lax.fori_loop(0, rows, attend, jnp.zeros((heads, LANES), f32))
    mlsend[...] = ml
    own_ml = pl.ds(pl.multiple_of(me * own_heads, 8), own_heads)
    mlbuf[me] = mlsend[own_ml, :]

    def send_ml(k, c):
        p_dev = peer_of(me, k, n_dev)
        pltpu.make_async_remote_copy(
            src_ref=mlsend.at[pl.ds(pl.multiple_of(p_dev * own_heads, 8), own_heads), :],
            dst_ref=mlbuf.at[me], send_sem=ml_ssem, recv_sem=ml_rsem,
            device_id={"model": p_dev}, device_id_type=pl.DeviceIdType.MESH).start()
        return c
    lax.fori_loop(1, n_dev, send_ml, 0, unroll=True)

    wait_bytes(kvbuf.at[pl.ds(0, n_dev - 1)], kv_rsem)
    kv_sum = kvbuf[0]
    for d in range(1, n_dev):
        kv_sum = kv_sum + kvbuf[d]
    kvout_v[...] = kv_sum.astype(bf16)
    k_write = pltpu.make_async_copy(kvout_v.at[0], k_out, out_sem.at[0])
    v_write = pltpu.make_async_copy(kvout_v.at[1], v_out, out_sem.at[1])
    k_write.start()
    v_write.start()
    k_new = kv_sum[0].astype(bf16).astype(f32)
    v_new = kv_sum[1].astype(bf16).astype(f32)

    wait_bytes(mlbuf.at[pl.ds(0, n_dev - 1)], ml_rsem)
    wait_bytes(obuf.at[pl.ds(0, n_dev - 1)], o_rsem)
    for b in range(rows):
        q_own = qbuf[pl.ds(me * own_heads, own_heads), b, :]
        s_new = jnp.sum(q_own * k_new[b:b + 1, :], axis=1, keepdims=True)
        top = s_new
        for d in range(n_dev):
            top = jnp.maximum(top, mlbuf[d, :, b:b + 1])
        w_new = jnp.exp2((s_new - top) * factor)
        total = w_new
        acc = w_new * v_new[b:b + 1, :]
        for d in range(n_dev):
            w_d = jnp.exp2((mlbuf[d, :, b:b + 1] - top) * factor)
            total = total + w_d * mlbuf[d, :, b + 8:b + 9]
            acc = acc + w_d * obuf[d, b]
        astage[b] = acc / total
    for h in range(own_heads):
        a_v[:, h * head_dim:(h + 1) * head_dim] = astage[:, h, :].astype(bf16)

    def y_step(j, c):
        wo_copy(j).wait()
        ysend[j] = jnp.dot(a_v[...], wo_v[j], preferred_element_type=f32)

        @pl.when(j < n_dev - 1)
        def _():
            pltpu.make_async_remote_copy(
                src_ref=ysend.at[j], dst_ref=ybuf.at[me], send_sem=y_ssem, recv_sem=y_rsem,
                device_id={"model": lax.rem(me + 1 + j, n_dev)},
                device_id_type=pl.DeviceIdType.MESH).start()
        return c
    lax.fori_loop(0, n_dev, y_step, 0)
    ybuf[me] = ysend[n_dev - 1]
    wait_bytes(ybuf.at[pl.ds(0, n_dev - 1)], y_rsem)
    y_sum = ybuf[0]
    for d in range(1, n_dev):
        y_sum = y_sum + ybuf[d]
    y_v[:, own_cols(me)] = (x_v[:, own_cols(me)].astype(f32) + y_sum).astype(bf16)
    send_all(y_v.at[:, own_cols(me)], y_v.at[:, own_cols(me)], g_ssem, g_rsem)
    wait_bytes(y_v.at[:, pl.ds(0, (n_dev - 1) * y_cols)], g_rsem)
    y_write = pltpu.make_async_copy(y_v, y_out, out_sem.at[2])
    y_write.start()

    wait_bytes(qbuf.at[pl.ds(0, heads - own_heads)], q_ssem)
    wait_bytes(kvbuf.at[pl.ds(0, n_dev - 1)], kv_ssem)
    wait_bytes(obuf.at[pl.ds(0, n_dev - 1)], o_ssem)
    wait_bytes(mlbuf.at[pl.ds(0, n_dev - 1)], ml_ssem)
    wait_bytes(ybuf.at[pl.ds(0, n_dev - 1)], y_ssem)
    wait_bytes(y_v.at[:, pl.ds(0, (n_dev - 1) * y_cols)], g_ssem)
    k_write.wait()
    v_write.wait()
    y_write.wait()


def solution(mesh):
    n_dev = mesh.shape["model"]

    def local_step(x, w_q, w_k, w_v, w_o, k_cache, v_cache, lengths):
        rows, _, t_local, head_dim = k_cache.shape
        depth = x.shape[1]
        own_heads = w_q.shape[1] // head_dim
        heads = own_heads * n_dev
        y_cols = w_o.shape[1] // n_dev
        kv_rows = depth // n_dev
        f32, bf16 = jnp.float32, jnp.bfloat16
        hbm = pl.BlockSpec(memory_space=pl.ANY)
        dma = pltpu.SemaphoreType.DMA
        return pl.pallas_call(
            functools.partial(kernel, n_dev),
            out_shape=(jax.ShapeDtypeStruct((rows, depth), bf16),
                       jax.ShapeDtypeStruct((rows, head_dim), bf16),
                       jax.ShapeDtypeStruct((rows, head_dim), bf16)),
            in_specs=[hbm] * 7 + [pl.BlockSpec(memory_space=pltpu.SMEM)],
            out_specs=(hbm, hbm, hbm),
            scratch_shapes=[
                pltpu.VMEM((rows, depth), bf16),
                pltpu.VMEM((RING, depth, head_dim), bf16),
                pltpu.VMEM((2, kv_rows, head_dim), bf16),
                pltpu.VMEM((rows, t_local, head_dim), bf16),
                pltpu.VMEM((rows, t_local, head_dim), bf16),
                pltpu.VMEM((n_dev, w_o.shape[0], y_cols), bf16),
                pltpu.VMEM((heads, rows, head_dim), f32),
                pltpu.VMEM((n_dev, 2, rows, head_dim), f32),
                pltpu.VMEM((rows, heads, head_dim), f32),
                pltpu.VMEM((n_dev, rows, own_heads, head_dim), f32),
                pltpu.VMEM((heads, LANES), f32),
                pltpu.VMEM((n_dev, own_heads, LANES), f32),
                pltpu.VMEM((rows, own_heads, head_dim), f32),
                pltpu.VMEM((rows, own_heads * head_dim), bf16),
                pltpu.VMEM((n_dev, rows, y_cols), f32),
                pltpu.VMEM((n_dev, rows, y_cols), f32),
                pltpu.VMEM((rows, depth), bf16),
                pltpu.VMEM((2, rows, head_dim), bf16),
                dma, dma((RING,)), dma((2,)), dma((rows,)), dma((rows,)), dma((n_dev,)), dma((3,)),
            ] + [dma] * 12,
            compiler_params=pltpu.CompilerParams(
                collective_id=0, has_side_effects=True, vmem_limit_bytes=67043328),
        )(x, w_q, w_k, w_v, w_o, k_cache, v_cache, lengths)

    row_spec = P("replica", None)
    cache_spec = P("replica", None, "model", None)
    return jax.shard_map(
        local_step, mesh=mesh,
        in_specs=(row_spec, P(None, "model"), P(), P(), P("model", None), cache_spec, cache_spec, P("replica")),
        out_specs=(row_spec, row_spec, row_spec), check_vma=False)
```

```python
import functools
import math

import jax
import jax.numpy as jnp
from jax import lax
from jax.experimental import pallas as pl
from jax.experimental.pallas import tpu as pltpu
from jax.sharding import PartitionSpec as P

RING = 4
LANES = 128
WIDE = 256
MESH = pl.DeviceIdType.MESH


def kernel(n_dev, x_hbm, wq_hbm, wk_hbm, wv_hbm, wo_hbm, kc_hbm, vc_hbm, len_hbm,
           y_out, k_out, v_out,
           len_s, x_v, w_v, wkv_v, k_v, v_v,
           qbuf, kvbuf, s_buf, osend, obuf, mlsend, mlbuf, astage, a_v, ysend, ybuf, y_v, kvout_v,
           len_sem, x_sem, wq_sem, wkv_sem, k_sem, v_sem, wo_sem, out_sem,
           q_ssem, q_rsem, kv_ssem, kv_rsem, o_ssem, o_rsem, ml_ssem, ml_rsem,
           y_ssem, y_rsem, g_ssem, g_rsem):
    rows, depth = x_hbm.shape
    head_dim = wk_hbm.shape[1]
    own_heads = wq_hbm.shape[1] // head_dim
    t_local = kc_hbm.shape[2]
    heads = own_heads * n_dev
    kv_rows = depth // n_dev
    y_cols = wo_hbm.shape[1] // n_dev
    o_rows = wo_hbm.shape[0]
    chips = n_dev // 2
    pieces = 2 * y_cols // WIDE
    ring_base = w_v.shape[0] - RING * depth
    me = lax.axis_index("model")
    chip, core = lax.div(me, 2), lax.rem(me, 2)
    factor = head_dim ** -0.5 * math.log2(math.e)
    f32, bf16 = jnp.float32, jnp.bfloat16

    def peer(d_chip, d_core):
        c_x = lax.rem(lax.rem(chip, 2) + d_chip % 2, 2)
        c_y = lax.rem(lax.div(chip, 2) + d_chip // 2, 2)
        return (c_y * 2 + c_x) * 2 + lax.rem(core + d_core, 2)

    peers = [peer(dc, dk) for dc, dk in ((3, 0), (3, 1), (1, 0), (2, 0), (1, 1), (2, 1), (0, 1))]

    def cols(i, width):
        return pl.ds(pl.multiple_of(i * width, LANES), width)

    def row_block(i, size):
        return pl.ds(pl.multiple_of(i * size, 8), size)

    def wq_slot(h):
        return pl.ds(pl.multiple_of(ring_base + lax.rem(h, RING) * depth, 256), depth)

    def wq_copy(h):
        return pltpu.make_async_copy(
            wq_hbm.at[:, cols(h, head_dim)], w_v.at[wq_slot(h), :], wq_sem.at[lax.rem(h, RING)])

    def wo_copy(g, i):
        c = lax.rem(chip + 1 + g, chips)
        piece = lax.rem(i + (pieces // 2) * (1 - core), pieces) if g == chips - 1 else i
        return pltpu.make_async_copy(
            wo_hbm.at[:, cols(c * pieces + piece, WIDE)],
            w_v.at[pl.ds((g * pieces + i) * o_rows, o_rows), :], wo_sem.at[g])

    def wait_bytes(ref, sem):
        pltpu.make_async_copy(ref, ref, sem).wait()

    def wait_group(g):
        wait_bytes(w_v.at[pl.ds(g * pieces * o_rows, pieces * o_rows), :], wo_sem.at[g])

    def send(src, dst, ssem, rsem, p):
        pltpu.make_async_remote_copy(
            src_ref=src, dst_ref=dst, send_sem=ssem, recv_sem=rsem,
            device_id={"model": p}, device_id_type=MESH).start()

    def send_all(ref, ssem, rsem):
        for p in peers:
            send(ref, ref, ssem, rsem, p)

    kv_slice = pl.ds(pl.multiple_of(me * kv_rows, LANES), kv_rows)
    x_copy = pltpu.make_async_copy(x_hbm, x_v, x_sem)
    len_copy = pltpu.make_async_copy(len_hbm, len_s, len_sem)
    wk_copy = pltpu.make_async_copy(wk_hbm.at[kv_slice, :], wkv_v.at[0], wkv_sem.at[0])
    wv_copy = pltpu.make_async_copy(wv_hbm.at[kv_slice, :], wkv_v.at[1], wkv_sem.at[1])
    k_copy = [pltpu.make_async_copy(kc_hbm.at[b, 0], k_v.at[b], k_sem.at[b]) for b in range(rows)]
    v_copy = [pltpu.make_async_copy(vc_hbm.at[b, 0], v_v.at[b], v_sem.at[b]) for b in range(rows)]

    x_copy.start()
    wq_copy(0).start()
    barrier = pltpu.get_barrier_semaphore()
    for p in peers:
        pl.semaphore_signal(barrier, inc=1, device_id={"model": p}, device_id_type=MESH)
    for h in range(1, RING):
        wq_copy(h).start()
    len_copy.start()
    with jax.named_scope('x_wait'):
        x_copy.wait()

    def q_step(h, c):
        with jax.named_scope('q_wait'):
            wq_copy(h).wait()
        q = jnp.dot(x_v[...], w_v[wq_slot(h), :], preferred_element_type=f32)
        block = me * own_heads + h
        qbuf[block] = q.astype(bf16).astype(f32)

        @pl.when(h == 0)
        def _():
            with jax.named_scope('barrier'):
                pl.semaphore_wait(barrier, n_dev - 1)

        send_all(qbuf.at[block], q_ssem, q_rsem)

        @pl.when(h < own_heads - RING)
        def _():
            wq_copy(h + RING).start()

        @pl.when(h == own_heads - RING)
        def _():
            wk_copy.start()
            wv_copy.start()
            for c in k_copy:
                c.start()

        @pl.when(h == own_heads - RING + 1)
        def _():
            for c in v_copy:
                c.start()

        @pl.when(h == own_heads - RING + 2)
        def _():
            for g in range(2):
                for i in range(pieces):
                    wo_copy(g, i).start()
        return c

    lax.fori_loop(0, own_heads, q_step, 0)
    for g in range(2, chips):
        for i in range(pieces):
            wo_copy(g, i).start()

    with jax.named_scope('wkv_wait'):
        wk_copy.wait()
        wv_copy.wait()
    x_part = x_v[:, kv_slice]
    for i in range(2):
        kvbuf[me, i] = jnp.dot(x_part, wkv_v[i], preferred_element_type=f32)
    send_all(kvbuf.at[me], kv_ssem, kv_rsem)

    with jax.named_scope('k_wait'):
        len_copy.wait()
        for c in k_copy:
            c.wait()
    with jax.named_scope('q_recv'):
        wait_bytes(qbuf.at[pl.ds(0, heads - own_heads)], q_rsem)

    positions = me * t_local + lax.broadcasted_iota(jnp.int32, (1, t_local), 1)
    lane = lax.broadcasted_iota(jnp.int32, (heads, LANES), 1)

    def scores(b):
        q_b = qbuf[:, b, :].astype(bf16)
        s_buf[b % 2] = lax.dot_general(q_b, k_v[b], (((1,), (1,)), ((), ())), preferred_element_type=f32)

    ml = jnp.zeros((heads, LANES), f32)
    scores(0)
    with jax.named_scope('v_wait'):
        for c in v_copy:
            c.wait()
    for b in range(rows):
        if b + 1 < rows:
            scores(b + 1)
        s = jnp.where(positions < len_s[b], s_buf[b % 2], -jnp.inf)
        m = jnp.max(s, axis=1, keepdims=True)
        m_safe = jnp.where(m == -jnp.inf, 0.0, m)
        p = jnp.exp2((s - m_safe) * factor)
        l = jnp.sum(p, axis=1, keepdims=True)
        hi = p.astype(bf16)
        lo = (p - hi.astype(f32)).astype(bf16)
        o2 = jnp.dot(jnp.concatenate([hi, lo], axis=0), v_v[b], preferred_element_type=f32)
        osend[b] = o2[:heads] + o2[heads:]
        obuf[me, b] = osend[b, row_block(me, own_heads), :]
        for d in peers:
            send(osend.at[b, row_block(d, own_heads), :], obuf.at[me, b], o_ssem, o_rsem, d)
        ml = jnp.where(lane == b, m, ml)
        ml = jnp.where(lane == b + 8, l, ml)
    mlsend[...] = ml
    mlbuf[me] = mlsend[row_block(me, own_heads), :]
    for d in peers:
        send(mlsend.at[row_block(d, own_heads), :], mlbuf.at[me], ml_ssem, ml_rsem, d)

    with jax.named_scope('kv_recv'):
        wait_bytes(kvbuf.at[pl.ds(0, n_dev - 1)], kv_rsem)
    kv_sum = kvbuf[0]
    for d in range(1, n_dev):
        kv_sum = kv_sum + kvbuf[d]
    kvout_v[...] = kv_sum.astype(bf16)
    k_write = pltpu.make_async_copy(kvout_v.at[0], k_out, out_sem.at[0])
    v_write = pltpu.make_async_copy(kvout_v.at[1], v_out, out_sem.at[1])
    k_write.start()
    v_write.start()
    k_new = kv_sum[0].astype(bf16).astype(f32)
    v_new = kv_sum[1].astype(bf16).astype(f32)

    with jax.named_scope('ml_recv'):
        wait_bytes(mlbuf.at[pl.ds(0, n_dev - 1)], ml_rsem)
    with jax.named_scope('o_recv'):
        wait_bytes(obuf.at[pl.ds(0, n_dev - 1)], o_rsem)
    for b in range(rows):
        q_own = qbuf[pl.ds(me * own_heads, own_heads), b, :]
        s_new = jnp.sum(q_own * k_new[b:b + 1, :], axis=1, keepdims=True)
        top = s_new
        for d in range(n_dev):
            top = jnp.maximum(top, mlbuf[d, :, b:b + 1])
        w_new = jnp.exp2((s_new - top) * factor)
        total = w_new
        acc = w_new * v_new[b:b + 1, :]
        for d in range(n_dev):
            w_d = jnp.exp2((mlbuf[d, :, b:b + 1] - top) * factor)
            total = total + w_d * mlbuf[d, :, b + 8:b + 9]
            acc = acc + w_d * obuf[d, b]
        astage[b] = acc / total
    for h in range(own_heads):
        a_v[:, h * head_dim:(h + 1) * head_dim] = astage[:, h, :].astype(bf16)

    def half(h):
        return pl.ds(pl.multiple_of(h * y_cols, LANES), y_cols)

    def y_piece(g, i, col):
        ysend[g, :, cols(col, WIDE)] = jnp.dot(
            a_v[...], w_v[pl.ds(pl.multiple_of((g * pieces + i) * o_rows, 256), o_rows), :],
            preferred_element_type=f32)

    def y_group(g, c):
        with jax.named_scope('wo_wait'):
            wait_group(g)
        target = 2 * lax.rem(chip + 1 + g, chips)
        for i in range(pieces):
            y_piece(g, i, i)
            if i == pieces // 2:
                send(ysend.at[g, :, half(0)], ybuf.at[me], y_ssem, y_rsem, target)
        send(ysend.at[g, :, half(1)], ybuf.at[me], y_ssem, y_rsem, target + 1)
        return c

    lax.fori_loop(0, chips - 1, y_group, 0)
    last = chips - 1
    with jax.named_scope('wo_wait'):
        wait_group(last)
    for i in range(pieces):
        y_piece(last, i, lax.rem(i + (pieces // 2) * (1 - core), pieces))
        if i == pieces // 2:
            send(ysend.at[last, :, half(1 - core)], ybuf.at[me], y_ssem, y_rsem, peers[-1])
    ybuf[me] = ysend[last, :, half(core)]
    with jax.named_scope('y_recv'):
        wait_bytes(ybuf.at[pl.ds(0, n_dev - 1)], y_rsem)
    y_sum = ybuf[0]
    for d in range(1, n_dev):
        y_sum = y_sum + ybuf[d]
    y_v[:, half(me)] = (x_v[:, half(me)].astype(f32) + y_sum).astype(bf16)
    send_all(y_v.at[:, half(me)], g_ssem, g_rsem)
    with jax.named_scope('g_recv'):
        wait_bytes(y_v.at[:, pl.ds(0, (n_dev - 1) * y_cols)], g_rsem)
    y_write = pltpu.make_async_copy(y_v, y_out, out_sem.at[2])
    y_write.start()

    wait_bytes(qbuf.at[pl.ds(0, heads - own_heads)], q_ssem)
    wait_bytes(kvbuf.at[pl.ds(0, n_dev - 1)], kv_ssem)
    wait_bytes(obuf.at[pl.ds(0, n_dev - 1)], o_ssem)
    wait_bytes(mlbuf.at[pl.ds(0, n_dev - 1)], ml_ssem)
    wait_bytes(ybuf.at[pl.ds(0, n_dev - 1)], y_ssem)
    wait_bytes(y_v.at[:, pl.ds(0, (n_dev - 1) * y_cols)], g_ssem)
    with jax.named_scope('out_wait'):
        k_write.wait()
        v_write.wait()
        y_write.wait()


def solution(mesh):
    n_dev = mesh.shape["model"]

    def local_step(x, w_q, w_k, w_v, w_o, k_cache, v_cache, lengths):
        rows, _, t_local, head_dim = k_cache.shape
        depth = x.shape[1]
        own_heads = w_q.shape[1] // head_dim
        heads = own_heads * n_dev
        y_cols = w_o.shape[1] // n_dev
        chips = n_dev // 2
        f32, bf16 = jnp.float32, jnp.bfloat16
        hbm = pl.BlockSpec(memory_space=pl.ANY)
        dma = pltpu.SemaphoreType.DMA
        return pl.pallas_call(
            functools.partial(kernel, n_dev),
            out_shape=(jax.ShapeDtypeStruct((rows, depth), bf16),
                       jax.ShapeDtypeStruct((rows, head_dim), bf16),
                       jax.ShapeDtypeStruct((rows, head_dim), bf16)),
            in_specs=[hbm] * 8,
            out_specs=(hbm, hbm, hbm),
            scratch_shapes=[
                pltpu.SMEM((rows,), jnp.int32),
                pltpu.VMEM((rows, depth), bf16),
                pltpu.VMEM((w_o.shape[0] * w_o.shape[1] // WIDE, WIDE), bf16),
                pltpu.VMEM((2, depth // n_dev, head_dim), bf16),
                pltpu.VMEM((rows, t_local, head_dim), bf16),
                pltpu.VMEM((rows, t_local, head_dim), bf16),
                pltpu.VMEM((heads, rows, head_dim), f32),
                pltpu.VMEM((n_dev, 2, rows, head_dim), f32),
                pltpu.VMEM((2, heads, t_local), f32),
                pltpu.VMEM((rows, heads, head_dim), f32),
                pltpu.VMEM((n_dev, rows, own_heads, head_dim), f32),
                pltpu.VMEM((heads, LANES), f32),
                pltpu.VMEM((n_dev, own_heads, LANES), f32),
                pltpu.VMEM((rows, own_heads, head_dim), f32),
                pltpu.VMEM((rows, own_heads * head_dim), bf16),
                pltpu.VMEM((chips, rows, 2 * y_cols), f32),
                pltpu.VMEM((n_dev, rows, y_cols), f32),
                pltpu.VMEM((rows, depth), bf16),
                pltpu.VMEM((2, rows, head_dim), bf16),
                dma, dma, dma((RING,)), dma((2,)), dma((rows,)), dma((rows,)), dma((chips,)), dma((3,)),
            ] + [dma] * 12,
            compiler_params=pltpu.CompilerParams(
                collective_id=0, has_side_effects=True, vmem_limit_bytes=67043328),
        )(x, w_q, w_k, w_v, w_o, k_cache, v_cache, lengths)

    row_spec = P("replica", None)
    cache_spec = P("replica", None, "model", None)
    return jax.shard_map(
        local_step, mesh=mesh,
        in_specs=(row_spec, P(None, "model"), P(), P(), P("model", None), cache_spec, cache_spec, P("replica")),
        out_specs=(row_spec, row_spec, row_spec), check_vma=False)
```

```python
import functools
import math

import jax
import jax.numpy as jnp
from jax import lax
from jax.experimental import pallas as pl
from jax.experimental.pallas import tpu as pltpu
from jax.sharding import PartitionSpec as P

RING = 4
LANES = 128
WIDE = 256
MESH = pl.DeviceIdType.MESH


def kernel(n_dev, x_hbm, wq_hbm, wk_hbm, wv_hbm, wo_hbm, kc_hbm, vc_hbm, len_hbm,
           y_out, k_out, v_out,
           len_s, x_v, w_v, wkv_v, k_v, v_v,
           qbuf, kvbuf, s_buf, osend, obuf, mlsend, mlbuf, astage, a_v, ysend, ybuf, y_v,
           len_sem, x_sem, wq_sem, wkv_sem, k_sem, v_sem, wo_sem,
           q_ssem, q_rsem, kv_ssem, kv_rsem, o_ssem, o_rsem, ml_ssem, ml_rsem,
           y_ssem, y_rsem, g_ssem, g_rsem):
    rows, depth = x_hbm.shape
    head_dim = wk_hbm.shape[1]
    own_heads = wq_hbm.shape[1] // head_dim
    t_local = kc_hbm.shape[2]
    heads = own_heads * n_dev
    kv_rows = depth // n_dev
    y_cols = wo_hbm.shape[1] // n_dev
    o_rows = wo_hbm.shape[0]
    chips = n_dev // 2
    pieces = 2 * y_cols // WIDE
    ring_base = w_v.shape[0] - RING * depth
    me = lax.axis_index("model")
    chip, core = lax.div(me, 2), lax.rem(me, 2)
    factor = head_dim ** -0.5 * math.log2(math.e)
    f32, bf16 = jnp.float32, jnp.bfloat16

    def peer(d_chip, d_core):
        c_x = lax.rem(lax.rem(chip, 2) + d_chip % 2, 2)
        c_y = lax.rem(lax.div(chip, 2) + d_chip // 2, 2)
        return (c_y * 2 + c_x) * 2 + lax.rem(core + d_core, 2)

    peers = [peer(dc, dk) for dc, dk in ((3, 0), (3, 1), (1, 0), (2, 0), (1, 1), (2, 1), (0, 1))]

    def cols(i, width):
        return pl.ds(pl.multiple_of(i * width, LANES), width)

    def row_block(i, size):
        return pl.ds(pl.multiple_of(i * size, 8), size)

    def wq_slot(h):
        return pl.ds(pl.multiple_of(ring_base + lax.rem(h, RING) * depth, 256), depth)

    def wq_copy(h):
        return pltpu.make_async_copy(
            wq_hbm.at[:, cols(h, head_dim)], w_v.at[wq_slot(h), :], wq_sem.at[lax.rem(h, RING)])

    def wo_copy(g, i):
        c = lax.rem(chip + 1 + g, chips)
        piece = lax.rem(i + (pieces // 2) * (1 - core), pieces) if g == chips - 1 else i
        return pltpu.make_async_copy(
            wo_hbm.at[:, cols(c * pieces + piece, WIDE)],
            w_v.at[pl.ds((g * pieces + i) * o_rows, o_rows), :], wo_sem.at[g])

    def wait_bytes(ref, sem):
        pltpu.make_async_copy(ref, ref, sem).wait()

    def wait_group(g):
        wait_bytes(w_v.at[pl.ds(g * pieces * o_rows, pieces * o_rows), :], wo_sem.at[g])

    def send(src, dst, ssem, rsem, p):
        pltpu.make_async_remote_copy(
            src_ref=src, dst_ref=dst, send_sem=ssem, recv_sem=rsem,
            device_id={"model": p}, device_id_type=MESH).start()

    def send_all(ref, ssem, rsem):
        for p in peers:
            send(ref, ref, ssem, rsem, p)

    kv_slice = pl.ds(pl.multiple_of(me * kv_rows, LANES), kv_rows)
    x_copy = pltpu.make_async_copy(x_hbm, x_v, x_sem)
    len_copy = pltpu.make_async_copy(len_hbm, len_s, len_sem)
    wk_copy = pltpu.make_async_copy(wk_hbm.at[kv_slice, :], wkv_v.at[0], wkv_sem.at[0])
    wv_copy = pltpu.make_async_copy(wv_hbm.at[kv_slice, :], wkv_v.at[1], wkv_sem.at[1])
    k_copy = [pltpu.make_async_copy(kc_hbm.at[b, 0], k_v.at[b], k_sem.at[b]) for b in range(rows)]
    v_copy = [pltpu.make_async_copy(vc_hbm.at[b, 0], v_v.at[b], v_sem.at[b]) for b in range(rows)]

    x_copy.start()
    wq_copy(0).start()
    barrier = pltpu.get_barrier_semaphore()
    for p in peers:
        pl.semaphore_signal(barrier, inc=1, device_id={"model": p}, device_id_type=MESH)
    for h in range(1, RING):
        wq_copy(h).start()
    len_copy.start()
    with jax.named_scope('x_wait'):
        x_copy.wait()

    def q_step(h, c):
        with jax.named_scope('q_wait'):
            wq_copy(h).wait()
        q = jnp.dot(x_v[...], w_v[wq_slot(h), :], preferred_element_type=f32)
        block = me * own_heads + h
        qbuf[block] = q.astype(bf16).astype(f32)

        @pl.when(h == 0)
        def _():
            with jax.named_scope('barrier'):
                pl.semaphore_wait(barrier, n_dev - 1)

        send_all(qbuf.at[block], q_ssem, q_rsem)

        @pl.when(h < own_heads - RING)
        def _():
            wq_copy(h + RING).start()

        @pl.when(h == own_heads - RING)
        def _():
            wk_copy.start()
            wv_copy.start()
            for c in k_copy:
                c.start()

        @pl.when(h == own_heads - RING + 1)
        def _():
            for c in v_copy:
                c.start()

        @pl.when(h == own_heads - RING + 2)
        def _():
            for g in range(2):
                for i in range(pieces):
                    wo_copy(g, i).start()
        return c

    lax.fori_loop(0, own_heads, q_step, 0)
    for g in range(2, chips):
        for i in range(pieces):
            wo_copy(g, i).start()

    with jax.named_scope('wkv_wait'):
        wk_copy.wait()
        wv_copy.wait()
    x_part = x_v[:, kv_slice]
    for i in range(2):
        kvbuf[me, i] = jnp.dot(x_part, wkv_v[i], preferred_element_type=f32)
    send_all(kvbuf.at[me], kv_ssem, kv_rsem)

    with jax.named_scope('k_wait'):
        len_copy.wait()
        for c in k_copy:
            c.wait()
    with jax.named_scope('q_recv'):
        wait_bytes(qbuf.at[pl.ds(0, heads - own_heads)], q_rsem)

    positions = me * t_local + lax.broadcasted_iota(jnp.int32, (1, t_local), 1)
    lane = lax.broadcasted_iota(jnp.int32, (heads, LANES), 1)

    def scores(b):
        q_b = qbuf[:, b, :].astype(bf16)
        s_buf[b % 2] = lax.dot_general(q_b, k_v[b], (((1,), (1,)), ((), ())), preferred_element_type=f32)

    ml = jnp.zeros((heads, LANES), f32)
    scores(0)
    with jax.named_scope('v_wait'):
        for c in v_copy:
            c.wait()
    for b in range(rows):
        if b + 1 < rows:
            scores(b + 1)
        s = jnp.where(positions < len_s[b], s_buf[b % 2], -jnp.inf)
        m = jnp.max(s, axis=1, keepdims=True)
        m_safe = jnp.where(m == -jnp.inf, 0.0, m)
        p = jnp.exp2((s - m_safe) * factor)
        l = jnp.sum(p, axis=1, keepdims=True)
        hi = p.astype(bf16)
        lo = (p - hi.astype(f32)).astype(bf16)
        o2 = jnp.dot(jnp.concatenate([hi, lo], axis=0), v_v[b], preferred_element_type=f32)
        osend[b] = o2[:heads] + o2[heads:]
        obuf[me, b] = osend[b, row_block(me, own_heads), :]
        for d in peers:
            send(osend.at[b, row_block(d, own_heads), :], obuf.at[me, b], o_ssem, o_rsem, d)
        ml = jnp.where(lane == b, m, ml)
        ml = jnp.where(lane == b + 8, l, ml)
    mlsend[...] = ml
    mlbuf[me] = mlsend[row_block(me, own_heads), :]
    for d in peers:
        send(mlsend.at[row_block(d, own_heads), :], mlbuf.at[me], ml_ssem, ml_rsem, d)

    with jax.named_scope('kv_recv'):
        wait_bytes(kvbuf.at[pl.ds(0, n_dev - 1)], kv_rsem)
    kv_sum = kvbuf[0]
    for d in range(1, n_dev):
        kv_sum = kv_sum + kvbuf[d]
    k_out[...] = kv_sum[0].astype(bf16)
    v_out[...] = kv_sum[1].astype(bf16)
    k_new = kv_sum[0].astype(bf16).astype(f32)
    v_new = kv_sum[1].astype(bf16).astype(f32)

    with jax.named_scope('ml_recv'):
        wait_bytes(mlbuf.at[pl.ds(0, n_dev - 1)], ml_rsem)
    with jax.named_scope('o_recv'):
        wait_bytes(obuf.at[pl.ds(0, n_dev - 1)], o_rsem)
    for b in range(rows):
        q_own = qbuf[pl.ds(me * own_heads, own_heads), b, :]
        s_new = jnp.sum(q_own * k_new[b:b + 1, :], axis=1, keepdims=True)
        top = s_new
        for d in range(n_dev):
            top = jnp.maximum(top, mlbuf[d, :, b:b + 1])
        w_new = jnp.exp2((s_new - top) * factor)
        total = w_new
        acc = w_new * v_new[b:b + 1, :]
        for d in range(n_dev):
            w_d = jnp.exp2((mlbuf[d, :, b:b + 1] - top) * factor)
            total = total + w_d * mlbuf[d, :, b + 8:b + 9]
            acc = acc + w_d * obuf[d, b]
        astage[b] = acc / total
    for h in range(own_heads):
        a_v[:, h * head_dim:(h + 1) * head_dim] = astage[:, h, :].astype(bf16)

    def half(h):
        return pl.ds(pl.multiple_of(h * y_cols, LANES), y_cols)

    def y_piece(g, i, col):
        ysend[g, :, cols(col, WIDE)] = jnp.dot(
            a_v[...], w_v[pl.ds(pl.multiple_of((g * pieces + i) * o_rows, 256), o_rows), :],
            preferred_element_type=f32)

    def y_group(g, c):
        with jax.named_scope('wo_wait'):
            wait_group(g)
        target = 2 * lax.rem(chip + 1 + g, chips)
        for i in range(pieces):
            y_piece(g, i, i)
            if i == pieces // 2:
                send(ysend.at[g, :, half(0)], ybuf.at[me], y_ssem, y_rsem, target)
        send(ysend.at[g, :, half(1)], ybuf.at[me], y_ssem, y_rsem, target + 1)
        return c

    lax.fori_loop(0, chips - 1, y_group, 0)
    last = chips - 1
    with jax.named_scope('wo_wait'):
        wait_group(last)
    for i in range(pieces):
        y_piece(last, i, lax.rem(i + (pieces // 2) * (1 - core), pieces))
        if i == pieces // 2:
            send(ysend.at[last, :, half(1 - core)], ybuf.at[me], y_ssem, y_rsem, peers[-1])
    ybuf[me] = ysend[last, :, half(core)]
    with jax.named_scope('y_recv'):
        wait_bytes(ybuf.at[pl.ds(0, n_dev - 1)], y_rsem)
    y_sum = ybuf[0]
    for d in range(1, n_dev):
        y_sum = y_sum + ybuf[d]
    y_v[:, half(me)] = (x_v[:, half(me)].astype(f32) + y_sum).astype(bf16)
    send_all(y_v.at[:, half(me)], g_ssem, g_rsem)
    with jax.named_scope('g_recv'):
        wait_bytes(y_v.at[:, pl.ds(0, (n_dev - 1) * y_cols)], g_rsem)
    y_out[...] = y_v[...]

    wait_bytes(qbuf.at[pl.ds(0, heads - own_heads)], q_ssem)
    wait_bytes(kvbuf.at[pl.ds(0, n_dev - 1)], kv_ssem)
    wait_bytes(obuf.at[pl.ds(0, n_dev - 1)], o_ssem)
    wait_bytes(mlbuf.at[pl.ds(0, n_dev - 1)], ml_ssem)
    wait_bytes(ybuf.at[pl.ds(0, n_dev - 1)], y_ssem)
    wait_bytes(y_v.at[:, pl.ds(0, (n_dev - 1) * y_cols)], g_ssem)


def store_kernel(*refs):
    sems, n_out = refs[-1], len(refs) // 2
    copies = [pltpu.make_async_copy(refs[i], refs[n_out + i], sems.at[i]) for i in range(n_out)]
    for c in copies:
        c.start()
    for c in copies:
        c.wait()


def solution(mesh):
    n_dev = mesh.shape["model"]

    def local_step(x, w_q, w_k, w_v, w_o, k_cache, v_cache, lengths):
        rows, _, t_local, head_dim = k_cache.shape
        depth = x.shape[1]
        own_heads = w_q.shape[1] // head_dim
        heads = own_heads * n_dev
        y_cols = w_o.shape[1] // n_dev
        chips = n_dev // 2
        f32, bf16 = jnp.float32, jnp.bfloat16
        hbm = pl.BlockSpec(memory_space=pl.ANY)
        dma = pltpu.SemaphoreType.DMA
        vm = pl.BlockSpec(memory_space=pltpu.VMEM)
        y, k_new, v_new = pl.pallas_call(
            functools.partial(kernel, n_dev),
            out_shape=(pltpu.VMEM((rows, depth), bf16),
                       pltpu.VMEM((rows, head_dim), bf16),
                       pltpu.VMEM((rows, head_dim), bf16)),
            in_specs=[hbm] * 8,
            out_specs=(vm, vm, vm),
            scratch_shapes=[
                pltpu.SMEM((rows,), jnp.int32),
                pltpu.VMEM((rows, depth), bf16),
                pltpu.VMEM((w_o.shape[0] * w_o.shape[1] // WIDE, WIDE), bf16),
                pltpu.VMEM((2, depth // n_dev, head_dim), bf16),
                pltpu.VMEM((rows, t_local, head_dim), bf16),
                pltpu.VMEM((rows, t_local, head_dim), bf16),
                pltpu.VMEM((heads, rows, head_dim), f32),
                pltpu.VMEM((n_dev, 2, rows, head_dim), f32),
                pltpu.VMEM((2, heads, t_local), f32),
                pltpu.VMEM((rows, heads, head_dim), f32),
                pltpu.VMEM((n_dev, rows, own_heads, head_dim), f32),
                pltpu.VMEM((heads, LANES), f32),
                pltpu.VMEM((n_dev, own_heads, LANES), f32),
                pltpu.VMEM((rows, own_heads, head_dim), f32),
                pltpu.VMEM((rows, own_heads * head_dim), bf16),
                pltpu.VMEM((chips, rows, 2 * y_cols), f32),
                pltpu.VMEM((n_dev, rows, y_cols), f32),
                pltpu.VMEM((rows, depth), bf16),
                dma, dma, dma((RING,)), dma((2,)), dma((rows,)), dma((rows,)), dma((chips,)),
            ] + [dma] * 12,
            compiler_params=pltpu.CompilerParams(
                collective_id=0, has_side_effects=True, vmem_limit_bytes=63000000),
        )(x, w_q, w_k, w_v, w_o, k_cache, v_cache, lengths)
        outs = (y, k_new, v_new)
        return pl.pallas_call(
            store_kernel,
            out_shape=tuple(jax.ShapeDtypeStruct(o.shape, o.dtype) for o in outs),
            in_specs=[hbm] * 3,
            out_specs=(hbm,) * 3,
            scratch_shapes=[dma((len(outs),))],
            compiler_params=pltpu.CompilerParams(vmem_limit_bytes=1 << 20),
        )(*outs)

    row_spec = P("replica", None)
    cache_spec = P("replica", None, "model", None)
    return jax.shard_map(
        local_step, mesh=mesh,
        in_specs=(row_spec, P(None, "model"), P(), P(), P("model", None), cache_spec, cache_spec, P("replica")),
        out_specs=(row_spec, row_spec, row_spec), check_vma=False)
```

```python
import functools
import math

import jax
import jax.numpy as jnp
from jax import lax
from jax.experimental import pallas as pl
from jax.experimental.pallas import tpu as pltpu
from jax.sharding import PartitionSpec as P

RING = 4
LANES = 128
WIDE = 256
FIRST = 5
BATCH = 3
SENDS = (3, 2)
MESH = pl.DeviceIdType.MESH


def kernel(n_dev, x_hbm, wq_hbm, wk_hbm, wv_hbm, wo_hbm, kc_hbm, vc_hbm, len_hbm,
           y_out, k_out, v_out,
           len_s, x_v, w_v, wkv_v, k_v, v_v, kvbuf, s_buf, yacc, ysend, ybuf, y_v, *rest):
    part_refs, sems = (rest[:9], rest[9:18]), rest[18:]
    (len_sem, x_sem, wq_sem, wkv_sem, k_sem, v_sem, wo_sem,
     kv_ssem, kv_rsem, y_ssem, y_rsem, g_ssem, g_rsem, q_ssem, q_rsem, o_ssem, o_rsem, ml_ssem, ml_rsem) = sems
    rows, depth = x_hbm.shape
    head_dim = wk_hbm.shape[1]
    own_heads = wq_hbm.shape[1] // head_dim
    t_local = kc_hbm.shape[2]
    kv_rows = depth // n_dev
    y_cols = wo_hbm.shape[1] // n_dev
    o_rows = wo_hbm.shape[0]
    chips = n_dev // 2
    pieces = 2 * y_cols // WIDE
    ring_base = w_v.shape[0] - RING * depth
    part_heads = (FIRST, own_heads - FIRST)
    part_row0 = (0, FIRST * head_dim)
    me = lax.axis_index("model")
    chip, core = lax.div(me, 2), lax.rem(me, 2)
    factor = head_dim ** -0.5 * math.log2(math.e)
    f32, bf16 = jnp.float32, jnp.bfloat16

    def chip_at(delta):
        c_x = lax.rem(lax.rem(chip, 2) + delta % 2, 2)
        c_y = lax.rem(lax.div(chip, 2) + delta // 2, 2)
        return c_y * 2 + c_x

    def peer(d_chip, d_core):
        return chip_at(d_chip) * 2 + lax.rem(core + d_core, 2)

    peers = [peer(dc, dk) for dc, dk in ((3, 0), (3, 1), (1, 0), (2, 0), (1, 1), (2, 1), (0, 1))]
    group_chip = [chip_at(d) for d in (3, 1, 2, 0)]

    def cols(i, width):
        return pl.ds(pl.multiple_of(i * width, LANES), width)

    def wq_slot(h):
        return pl.ds(pl.multiple_of(ring_base + lax.rem(h, RING) * depth, 256), depth)

    def wq_copy(h):
        return pltpu.make_async_copy(
            wq_hbm.at[:, cols(h, head_dim)], w_v.at[wq_slot(h), :], wq_sem.at[lax.rem(h, RING)])

    def wo_copy(part, g, i):
        size = part_heads[part] * head_dim
        return pltpu.make_async_copy(
            wo_hbm.at[pl.ds(part_row0[part], size), cols(group_chip[g] * pieces + i, WIDE)],
            w_v.at[pl.ds((g * pieces + i) * o_rows + part_row0[part], size), :], wo_sem.at[part, g])

    def wait_bytes(ref, sem):
        pltpu.make_async_copy(ref, ref, sem).wait()

    def wait_group(part, g):
        wait_bytes(w_v.at[pl.ds(0, pieces * part_heads[part] * head_dim), :], wo_sem.at[part, g])

    def send(src, dst, ssem, rsem, p):
        pltpu.make_async_remote_copy(
            src_ref=src, dst_ref=dst, send_sem=ssem, recv_sem=rsem,
            device_id={"model": p}, device_id_type=MESH).start()

    def send_all(ref, ssem, rsem):
        for p in peers:
            send(ref, ref, ssem, rsem, p)

    kv_slice = pl.ds(pl.multiple_of(me * kv_rows, LANES), kv_rows)
    x_copy = pltpu.make_async_copy(x_hbm, x_v, x_sem)
    len_copy = pltpu.make_async_copy(len_hbm, len_s, len_sem)
    wk_copy = pltpu.make_async_copy(wk_hbm.at[kv_slice, :], wkv_v.at[0], wkv_sem.at[0])
    wv_copy = pltpu.make_async_copy(wv_hbm.at[kv_slice, :], wkv_v.at[1], wkv_sem.at[1])

    def k_copy(b):
        return pltpu.make_async_copy(kc_hbm.at[b, 0], k_v.at[b], k_sem.at[b])

    def v_copy(b):
        return pltpu.make_async_copy(vc_hbm.at[b, 0], v_v.at[b], v_sem.at[b])

    x_copy.start()
    wq_copy(0).start()
    barrier = pltpu.get_barrier_semaphore()
    for p in peers:
        pl.semaphore_signal(barrier, inc=1, device_id={"model": p}, device_id_type=MESH)
    for h in range(1, RING):
        wq_copy(h).start()
    len_copy.start()
    with jax.named_scope('x_wait'):
        x_copy.wait()

    def q_loop(part):
        q_buf, n_heads = part_refs[part][0], part_heads[part]
        h0 = 0 if part == 0 else FIRST

        def q_step(h, c):
            with jax.named_scope('q_wait'):
                wq_copy(h).wait()
            q = jnp.dot(x_v[...], w_v[wq_slot(h), :], preferred_element_type=f32)
            block = me * n_heads + h - h0
            q_buf[block] = q.astype(bf16).astype(f32)
            if part == 0:
                @pl.when(h == 0)
                def _():
                    with jax.named_scope('barrier'):
                        pl.semaphore_wait(barrier, n_dev - 1)

            send_all(q_buf.at[block], q_ssem.at[part], q_rsem.at[part])
            if h0 < own_heads - RING:
                @pl.when(h < own_heads - RING)
                def _():
                    wq_copy(h + RING).start()

            if h0 <= own_heads - RING < h0 + n_heads:
                @pl.when(h == own_heads - RING)
                def _():
                    wk_copy.start()
                    wv_copy.start()

            if h0 <= own_heads - RING + 1 < h0 + n_heads:
                @pl.when(h == own_heads - RING + 1)
                def _():
                    def start_kv(b, c):
                        k_copy(b).start()
                        v_copy(b).start()
                        return c
                    lax.fori_loop(0, rows, start_kv, 0)
            return c

        lax.fori_loop(h0, h0 + n_heads, q_step, 0)

    q_loop(0)
    q_loop(1)
    for part in range(2):
        for g in range(chips):
            for i in range(pieces):
                wo_copy(part, g, i).start()

    positions = me * t_local + lax.broadcasted_iota(jnp.int32, (1, t_local), 1)

    def part_rows(part, b):
        n = (b % SENDS[part]) * part_heads[part]
        return slice(n, n + part_heads[part])

    def attention(part):
        q_buf, o_flat, osend, obuf, mlflat, mlsend, mlbuf = part_refs[part][:7]
        n_heads = part_heads[part]
        n_rows = n_heads * n_dev
        batch = SENDS[part]
        lane = lax.broadcasted_iota(jnp.int32, (n_rows, LANES), 1)

        def scores(b):
            q_b = q_buf[:, b, :].astype(bf16)
            s_buf[b % 3, 0:n_rows] = lax.dot_general(
                q_b, k_v[b], (((1,), (1,)), ((), ())), preferred_element_type=f32)

        def wait_kv(b0):
            with jax.named_scope('kv_wait'):
                for b in range(b0, b0 + BATCH):
                    k_copy(b).wait()
                    v_copy(b).wait()

        with jax.named_scope('q_recv'):
            wait_bytes(q_buf.at[pl.ds(0, n_rows - n_heads)], q_rsem.at[part])
        if part == 0:
            len_copy.wait()
            wait_kv(0)
        m_all = jnp.zeros((n_rows, LANES), f32)
        l_all = jnp.zeros((n_rows, LANES), f32)
        scores(0)
        for b in range(rows):
            if b + 1 < rows:
                if part == 0 and (b + 1) % BATCH == 0:
                    wait_kv(b + 1)
                scores(b + 1)
            s = jnp.where(positions < len_s[b], s_buf[b % 3, 0:n_rows], -jnp.inf)
            m = jnp.max(s, axis=1, keepdims=True)
            m_safe = jnp.where(m == -jnp.inf, 0.0, m)
            p = jnp.exp2((s - m_safe) * factor)
            l = jnp.sum(p, axis=1, keepdims=True)
            hi = p.astype(bf16).astype(f32)
            terms = jnp.concatenate([hi, p - hi], axis=0).astype(bf16)
            o2 = jnp.dot(terms, v_v[b], preferred_element_type=f32)
            o_flat[b] = o2[:n_rows] + o2[n_rows:]
            m_all = jnp.where(lane == b, m, m_all)
            l_all = jnp.where(lane == b, l, l_all)
            for d in range(n_dev):
                osend[b // batch, d, part_rows(part, b), :] = o_flat[b, d * n_heads:(d + 1) * n_heads, :]
            if (b + 1) % batch == 0:
                n = b // batch
                obuf[me, n] = osend[n, me]
                for d in peers:
                    send(osend.at[n, d], obuf.at[me, n], o_ssem.at[part], o_rsem.at[part], d)
        mlflat[0] = m_all
        mlflat[1] = l_all
        for d in range(n_dev):
            mlsend[d] = mlflat[:, d * n_heads:(d + 1) * n_heads, :]
        mlbuf[me] = mlsend[me]
        for d in peers:
            send(mlsend.at[d], mlbuf.at[me], ml_ssem.at[part], ml_rsem.at[part], d)

    with jax.named_scope('wkv_wait'):
        wk_copy.wait()
        wv_copy.wait()
    x_part = x_v[:, kv_slice]
    for i in range(2):
        kvbuf[me, i] = jnp.dot(x_part, wkv_v[i], preferred_element_type=f32)
    send_all(kvbuf.at[me], kv_ssem, kv_rsem)
    attention(0)
    attention(1)

    with jax.named_scope('kv_recv'):
        wait_bytes(kvbuf.at[pl.ds(0, n_dev - 1)], kv_rsem)
    kv_sum = kvbuf[0]
    for d in range(1, n_dev):
        kv_sum = kv_sum + kvbuf[d]
    k_out[...] = kv_sum[0].astype(bf16)
    v_out[...] = kv_sum[1].astype(bf16)
    k_new = kv_sum[0].astype(bf16).astype(f32)
    v_new = kv_sum[1].astype(bf16).astype(f32)

    def combine(part):
        q_buf, _, _, obuf, _, _, mlbuf, a_v, astage = part_refs[part]
        n_heads = part_heads[part]
        lane = lax.broadcasted_iota(jnp.int32, (n_heads, LANES), 1)
        with jax.named_scope('o_recv'):
            wait_bytes(mlbuf.at[pl.ds(0, n_dev - 1)], ml_rsem.at[part])
            wait_bytes(obuf.at[pl.ds(0, n_dev - 1)], o_rsem.at[part])
        s_new = jnp.zeros((n_heads, LANES), f32)
        for b in range(rows):
            q_own = q_buf[pl.ds(me * n_heads, n_heads), b, :]
            s_new = jnp.where(lane == b, jnp.sum(q_own * k_new[b:b + 1, :], axis=1, keepdims=True), s_new)
        top = s_new
        for d in range(n_dev):
            top = jnp.maximum(top, mlbuf[d, 0])
        w_new = jnp.exp2((s_new - top) * factor)
        w = [jnp.exp2((mlbuf[d, 0] - top) * factor) for d in range(n_dev)]
        total = w_new
        for d in range(n_dev):
            total = total + w[d] * mlbuf[d, 1]
        inv = 1.0 / total
        w_new = w_new * inv
        w = [w_d * inv for w_d in w]
        for b in range(rows):
            acc = w_new[:, b:b + 1] * v_new[b:b + 1, :]
            for d in range(n_dev):
                acc = acc + w[d][:, b:b + 1] * obuf[d, b // SENDS[part], part_rows(part, b), :]
            astage[b] = acc
        for h in range(n_heads):
            a_v[:, h * head_dim:(h + 1) * head_dim] = astage[:, h, :].astype(bf16)

    y_blocks = y_cols // LANES

    def y_rows_at(block):
        return slice(block * rows, (block + 1) * rows)

    def y_rows(part, g):
        a_v = part_refs[part][7]
        size = part_heads[part] * head_dim
        for i in range(pieces):
            row = pl.multiple_of((g * pieces + i) * o_rows + part_row0[part], 256)
            y = jnp.dot(a_v[...], w_v[pl.ds(row, size), :], preferred_element_type=f32)
            at = slice(i * WIDE, (i + 1) * WIDE)
            if part == 0:
                yacc[g, :, at] = y
                continue
            y = yacc[g, :, at] + y
            for j in range(WIDE // LANES):
                block = i * (WIDE // LANES) + j
                ysend[g, block // y_blocks, y_rows_at(block % y_blocks), :] = y[:, j * LANES:(j + 1) * LANES]

    def half(h):
        return pl.ds(pl.multiple_of(h * y_cols, LANES), y_cols)

    combine(0)

    def y_first(g, c):
        with jax.named_scope('wo_wait'):
            wait_group(0, g)
        y_rows(0, g)
        return c

    lax.fori_loop(0, chips, y_first, 0)
    combine(1)
    last = chips - 1
    for g in range(chips):
        with jax.named_scope('wo_wait'):
            wait_group(1, g)
        y_rows(1, g)
        if g < last:
            for k in range(2):
                send(ysend.at[g, k], ybuf.at[me], y_ssem, y_rsem, 2 * group_chip[g] + k)
    send(ysend.at[last, 1 - core], ybuf.at[me], y_ssem, y_rsem, peers[-1])
    ybuf[me] = ysend[last, core]
    with jax.named_scope('y_recv'):
        wait_bytes(ybuf.at[pl.ds(0, n_dev - 1)], y_rsem)
    y_sum = ybuf[0]
    for d in range(1, n_dev):
        y_sum = y_sum + ybuf[d]
    for j in range(y_blocks):
        at = pl.ds(pl.multiple_of(me * y_cols + j * LANES, LANES), LANES)
        y_v[:, at] = (x_v[:, at].astype(f32) + y_sum[y_rows_at(j), :]).astype(bf16)
    send_all(y_v.at[:, half(me)], g_ssem, g_rsem)
    with jax.named_scope('g_recv'):
        wait_bytes(y_v.at[:, pl.ds(0, (n_dev - 1) * y_cols)], g_rsem)
    y_out[...] = y_v[...]

    for part in range(2):
        q_buf, _, _, obuf, _, _, mlbuf = part_refs[part][:7]
        n_heads = part_heads[part]
        wait_bytes(q_buf.at[pl.ds(0, (n_dev - 1) * n_heads)], q_ssem.at[part])
        wait_bytes(obuf.at[pl.ds(0, n_dev - 1)], o_ssem.at[part])
        wait_bytes(mlbuf.at[pl.ds(0, n_dev - 1)], ml_ssem.at[part])
    wait_bytes(kvbuf.at[pl.ds(0, n_dev - 1)], kv_ssem)
    wait_bytes(ybuf.at[pl.ds(0, n_dev - 1)], y_ssem)
    wait_bytes(y_v.at[:, pl.ds(0, (n_dev - 1) * y_cols)], g_ssem)


def store_kernel(*refs):
    sems, n_out = refs[-1], len(refs) // 2
    copies = [pltpu.make_async_copy(refs[i], refs[n_out + i], sems.at[i]) for i in range(n_out)]
    for c in copies:
        c.start()
    for c in copies:
        c.wait()


def solution(mesh):
    n_dev = mesh.shape["model"]

    def local_step(x, w_q, w_k, w_v, w_o, k_cache, v_cache, lengths):
        rows, _, t_local, head_dim = k_cache.shape
        depth = x.shape[1]
        own_heads = w_q.shape[1] // head_dim
        y_cols = w_o.shape[1] // n_dev
        chips = n_dev // 2
        f32, bf16 = jnp.float32, jnp.bfloat16

        def part_scratch(n_heads, batch):
            return [
                pltpu.VMEM((n_dev * n_heads, rows, head_dim), f32),
                pltpu.VMEM((rows, n_dev * n_heads, head_dim), f32),
                pltpu.VMEM((rows // batch, n_dev, batch * n_heads, head_dim), f32),
                pltpu.VMEM((n_dev, rows // batch, batch * n_heads, head_dim), f32),
                pltpu.VMEM((2, n_dev * n_heads, LANES), f32),
                pltpu.VMEM((n_dev, 2, n_heads, LANES), f32),
                pltpu.VMEM((n_dev, 2, n_heads, LANES), f32),
                pltpu.VMEM((rows, n_heads * head_dim), bf16),
                pltpu.VMEM((rows, n_heads, head_dim), f32),
            ]

        hbm = pl.BlockSpec(memory_space=pl.ANY)
        dma = pltpu.SemaphoreType.DMA
        vm = pl.BlockSpec(memory_space=pltpu.VMEM)
        y, k_new, v_new = pl.pallas_call(
            functools.partial(kernel, n_dev),
            out_shape=(pltpu.VMEM((rows, depth), bf16),
                       pltpu.VMEM((rows, head_dim), bf16),
                       pltpu.VMEM((rows, head_dim), bf16)),
            in_specs=[hbm] * 8,
            out_specs=(vm, vm, vm),
            scratch_shapes=[
                pltpu.SMEM((rows,), jnp.int32),
                pltpu.VMEM((rows, depth), bf16),
                pltpu.VMEM((w_o.shape[0] * w_o.shape[1] // WIDE, WIDE), bf16),
                pltpu.VMEM((2, depth // n_dev, head_dim), bf16),
                pltpu.VMEM((rows, t_local, head_dim), bf16),
                pltpu.VMEM((rows, t_local, head_dim), bf16),
                pltpu.VMEM((n_dev, 2, rows, head_dim), f32),
                pltpu.VMEM((3, FIRST * n_dev, t_local), f32),
                pltpu.VMEM((chips, rows, 2 * y_cols), f32),
                pltpu.VMEM((chips, 2, rows * y_cols // LANES, LANES), f32),
                pltpu.VMEM((n_dev, rows * y_cols // LANES, LANES), f32),
                pltpu.VMEM((rows, depth), bf16),
                *part_scratch(FIRST, SENDS[0]), *part_scratch(own_heads - FIRST, SENDS[1]),
                dma, dma, dma((RING,)), dma((2,)), dma((rows,)), dma((rows,)), dma((2, chips)),
            ] + [dma] * 6 + [dma((2,))] * 6,
            compiler_params=pltpu.CompilerParams(
                collective_id=0, has_side_effects=True, vmem_limit_bytes=63000000),
        )(x, w_q, w_k, w_v, w_o, k_cache, v_cache, lengths)
        outs = (y, k_new, v_new)
        return pl.pallas_call(
            store_kernel,
            out_shape=tuple(jax.ShapeDtypeStruct(o.shape, o.dtype) for o in outs),
            in_specs=[hbm] * 3,
            out_specs=(hbm,) * 3,
            scratch_shapes=[dma((len(outs),))],
            compiler_params=pltpu.CompilerParams(vmem_limit_bytes=1 << 20),
        )(*outs)

    row_spec = P("replica", None)
    cache_spec = P("replica", None, "model", None)
    return jax.shard_map(
        local_step, mesh=mesh,
        in_specs=(row_spec, P(None, "model"), P(), P(), P("model", None), cache_spec, cache_spec, P("replica")),
        out_specs=(row_spec, row_spec, row_spec), check_vma=False)
```

```python
import functools
import math

import jax
import jax.numpy as jnp
from jax import lax
from jax.experimental import pallas as pl
from jax.experimental.pallas import tpu as pltpu
from jax.sharding import PartitionSpec as P

RING = 4
LANES = 128
WIDE = 256
FIRST = 4
SENDS = (2, 2)
MESH = pl.DeviceIdType.MESH


def kernel(n_dev, x_hbm, wq_hbm, wk_hbm, wv_hbm, wo_hbm, kc_hbm, vc_hbm, len_hbm,
           y_out, k_out, v_out,
           len_s, x_v, w_v, wkv_v, k_v, v_v, kt_v, kvbuf, s_buf, yacc, ysend, ybuf, y_v, *rest):
    part_refs, sems = (rest[:9], rest[9:18]), rest[18:]
    (len_sem, x_sem, wq_sem, wkv_sem, k_sem, v_sem, wo_sem,
     kv_ssem, kv_rsem, y_ssem, y_rsem, g_ssem, g_rsem, q_ssem, q_rsem, o_ssem, o_rsem, ml_ssem, ml_rsem) = sems
    rows, depth = x_hbm.shape
    head_dim = wk_hbm.shape[1]
    own_heads = wq_hbm.shape[1] // head_dim
    t_local = kc_hbm.shape[2]
    y_cols = wo_hbm.shape[1] // n_dev
    o_rows = wo_hbm.shape[0]
    chips = n_dev // 2
    pieces = 2 * y_cols // WIDE
    ring_base = w_v.shape[0] - RING * depth
    part_heads = (FIRST, own_heads - FIRST)
    part_row0 = (0, FIRST * head_dim)
    me = lax.axis_index("model")
    chip, core = lax.div(me, 2), lax.rem(me, 2)
    factor = head_dim ** -0.5 * math.log2(math.e)
    f32, bf16 = jnp.float32, jnp.bfloat16

    def chip_at(delta):
        c_x = lax.rem(lax.rem(chip, 2) + delta % 2, 2)
        c_y = lax.rem(lax.div(chip, 2) + delta // 2, 2)
        return c_y * 2 + c_x

    def peer(d_chip, d_core):
        return chip_at(d_chip) * 2 + lax.rem(core + d_core, 2)

    peers = [peer(dc, dk) for dc, dk in ((3, 0), (3, 1), (1, 0), (2, 0), (1, 1), (2, 1), (0, 1))]
    group_chip = [chip_at(d) for d in (3, 1, 2, 0)]

    def cols(i, width):
        return pl.ds(pl.multiple_of(i * width, LANES), width)

    def wq_slot(h):
        return pl.ds(pl.multiple_of(ring_base + lax.rem(h, RING) * depth, 256), depth)

    def wq_copy(h):
        return pltpu.make_async_copy(
            wq_hbm.at[:, cols(h, head_dim)], w_v.at[wq_slot(h), :], wq_sem.at[lax.rem(h, RING)])

    def wo_copy(part, g, i):
        size = part_heads[part] * head_dim
        return pltpu.make_async_copy(
            wo_hbm.at[pl.ds(part_row0[part], size), cols(group_chip[g] * pieces + i, WIDE)],
            w_v.at[pl.ds((g * pieces + i) * o_rows + part_row0[part], size), :], wo_sem.at[part, g])

    def wait_bytes(ref, sem):
        pltpu.make_async_copy(ref, ref, sem).wait()

    def wait_group(part, g):
        wait_bytes(w_v.at[pl.ds(0, pieces * part_heads[part] * head_dim), :], wo_sem.at[part, g])

    def send(src, dst, ssem, rsem, p):
        pltpu.make_async_remote_copy(
            src_ref=src, dst_ref=dst, send_sem=ssem, recv_sem=rsem,
            device_id={"model": p}, device_id_type=MESH).start()

    def send_all(ref, ssem, rsem):
        for p in peers:
            send(ref, ref, ssem, rsem, p)

    x_copy = pltpu.make_async_copy(x_hbm, x_v, x_sem)
    len_copy = pltpu.make_async_copy(len_hbm, len_s, len_sem)
    wk_copy = pltpu.make_async_copy(wk_hbm, wkv_v, wkv_sem)
    wv_copy = pltpu.make_async_copy(wv_hbm, wkv_v, wkv_sem)

    def k_copy(b):
        return pltpu.make_async_copy(kc_hbm.at[b, 0], k_v.at[b], k_sem.at[b])

    def v_copy(b):
        return pltpu.make_async_copy(vc_hbm.at[b, 0], v_v.at[b], v_sem.at[b])

    x_copy.start()
    wq_copy(0).start()
    barrier = pltpu.get_barrier_semaphore()
    for p in peers:
        pl.semaphore_signal(barrier, inc=1, device_id={"model": p}, device_id_type=MESH)
    for h in range(1, RING):
        wq_copy(h).start()
    len_copy.start()
    with jax.named_scope('x_wait'):
        x_copy.wait()

    def q_loop(part):
        q_buf, n_heads = part_refs[part][0], part_heads[part]
        h0 = 0 if part == 0 else FIRST

        def q_step(h, c):
            with jax.named_scope('q_wait'):
                wq_copy(h).wait()
            q = jnp.dot(x_v[...], w_v[wq_slot(h), :], preferred_element_type=f32)
            block = me * n_heads + h - h0
            q_buf[block] = q.astype(bf16).astype(f32)
            if part == 0:
                @pl.when(h == 0)
                def _():
                    with jax.named_scope('barrier'):
                        pl.semaphore_wait(barrier, n_dev - 1)

            send_all(q_buf.at[block], q_ssem.at[part], q_rsem.at[part])
            if h0 < own_heads - RING:
                @pl.when(h < own_heads - RING)
                def _():
                    wq_copy(h + RING).start()

            if part == 1:
                @pl.when((h == h0) & (me == 0))
                def _():
                    wk_copy.start()

                @pl.when((h == h0) & (me == 1))
                def _():
                    wv_copy.start()

                @pl.when(h == h0 + 1)
                def _():
                    def start_kv(b, c):
                        k_copy(b).start()
                        v_copy(b).start()
                        return c
                    lax.fori_loop(0, rows, start_kv, 0)
            return c

        lax.fori_loop(h0, h0 + n_heads, q_step, 0)

    q_loop(0)
    q_loop(1)
    for part in range(2):
        for g in range(chips):
            for i in range(pieces):
                wo_copy(part, g, i).start()

    positions = me * t_local + lax.broadcasted_iota(jnp.int32, (1, t_local), 1)

    def part_rows(part, b):
        n = (b % SENDS[part]) * part_heads[part]
        return slice(n, n + part_heads[part])

    def attention(part):
        q_buf, o_flat, osend, obuf, mlflat, mlsend, mlbuf = part_refs[part][:7]
        n_heads = part_heads[part]
        n_rows = n_heads * n_dev
        batch = SENDS[part]
        lane = lax.broadcasted_iota(jnp.int32, (n_rows, LANES), 1)

        def scores(b):
            q_b = q_buf[:, b, :].astype(bf16)
            if part == 0:
                kt_v[b] = k_v[b].T
                s_buf[b % 3] = lax.dot_general(
                    q_b, k_v[b], (((1,), (1,)), ((), ())), preferred_element_type=f32)
            else:
                s_buf[b % 3] = jnp.dot(q_b, kt_v[b], preferred_element_type=f32)

        with jax.named_scope('q_recv'):
            wait_bytes(q_buf.at[pl.ds(0, n_rows - n_heads)], q_rsem.at[part])
        m_all = jnp.zeros((n_rows, LANES), f32)
        l_all = jnp.zeros((n_rows, LANES), f32)
        if part == 0:
            len_copy.wait()
        else:
            scores(0)
            scores(1)
        for b in range(rows):
            if part == 0 and b % batch == 0:
                with jax.named_scope('kv_wait'):
                    for c in range(b, b + batch):
                        k_copy(c).wait()
                        v_copy(c).wait()
                for c in range(b, b + batch):
                    scores(c)
            if part == 1 and b + 2 < rows:
                scores(b + 2)
            s = jnp.where(positions < len_s[b], s_buf[b % 3], -jnp.inf)
            m = jnp.max(s, axis=1, keepdims=True)
            m_safe = jnp.where(m == -jnp.inf, 0.0, m)
            p = jnp.exp2((s - m_safe) * factor)
            l = jnp.sum(p, axis=1, keepdims=True)
            hi = p.astype(bf16).astype(f32)
            terms = jnp.concatenate([hi, p - hi], axis=0).astype(bf16)
            o2 = jnp.dot(terms, v_v[b], preferred_element_type=f32)
            o_flat[b] = o2[:n_rows] + o2[n_rows:]
            m_all = jnp.where(lane == b, m, m_all)
            l_all = jnp.where(lane == b, l, l_all)
            for d in range(n_dev):
                osend[b // batch, d, part_rows(part, b), :] = o_flat[b, d * n_heads:(d + 1) * n_heads, :]
            if (b + 1) % batch == 0:
                n = b // batch
                obuf[me, n] = osend[n, me]
                for d in peers:
                    send(osend.at[n, d], obuf.at[me, n], o_ssem.at[part], o_rsem.at[part], d)
        mlflat[0] = m_all
        mlflat[1] = l_all
        for d in range(n_dev):
            mlsend[d] = mlflat[:, d * n_heads:(d + 1) * n_heads, :]
        mlbuf[me] = mlsend[me]
        for d in peers:
            send(mlsend.at[d], mlbuf.at[me], ml_ssem.at[part], ml_rsem.at[part], d)

    @pl.when(me < 2)
    def _():
        with jax.named_scope('wkv_wait'):
            wk_copy.wait()
        kv = jnp.dot(x_v[...], wkv_v[...], preferred_element_type=f32)
        kvbuf[me] = kv.astype(bf16).astype(f32)
        for p in peers:
            send(kvbuf.at[me], kvbuf.at[me], kv_ssem, kv_rsem.at[me], p)

    attention(0)
    attention(1)

    for i in range(2):
        @pl.when(me != i)
        def _():
            with jax.named_scope('kv_recv'):
                wait_bytes(kvbuf.at[i], kv_rsem.at[i])
    k_new, v_new = kvbuf[0], kvbuf[1]
    k_out[...] = k_new.astype(bf16)
    v_out[...] = v_new.astype(bf16)

    def combine(part):
        q_buf, _, _, obuf, _, _, mlbuf, a_v, astage = part_refs[part]
        n_heads = part_heads[part]
        lane = lax.broadcasted_iota(jnp.int32, (n_heads, LANES), 1)
        with jax.named_scope('o_recv'):
            wait_bytes(mlbuf.at[pl.ds(0, n_dev - 1)], ml_rsem.at[part])
            wait_bytes(obuf.at[pl.ds(0, n_dev - 1)], o_rsem.at[part])
        s_new = jnp.zeros((n_heads, LANES), f32)
        for b in range(rows):
            q_own = q_buf[pl.ds(me * n_heads, n_heads), b, :]
            s_new = jnp.where(lane == b, jnp.sum(q_own * k_new[b:b + 1, :], axis=1, keepdims=True), s_new)
        top = s_new
        for d in range(n_dev):
            top = jnp.maximum(top, mlbuf[d, 0])
        w_new = jnp.exp2((s_new - top) * factor)
        w = [jnp.exp2((mlbuf[d, 0] - top) * factor) for d in range(n_dev)]
        total = w_new
        for d in range(n_dev):
            total = total + w[d] * mlbuf[d, 1]
        inv = 1.0 / total
        w_new = w_new * inv
        w = [w_d * inv for w_d in w]
        for b in range(rows):
            acc = w_new[:, b:b + 1] * v_new[b:b + 1, :]
            for d in range(n_dev):
                acc = acc + w[d][:, b:b + 1] * obuf[d, b // SENDS[part], part_rows(part, b), :]
            astage[b] = acc
        for h in range(n_heads):
            a_v[:, h * head_dim:(h + 1) * head_dim] = astage[:, h, :].astype(bf16)

    y_blocks = y_cols // LANES

    def y_rows_at(block):
        return slice(block * rows, (block + 1) * rows)

    def y_rows(part, g):
        a_v = part_refs[part][7]
        size = part_heads[part] * head_dim
        for i in range(pieces):
            row = pl.multiple_of((g * pieces + i) * o_rows + part_row0[part], 256)
            y = jnp.dot(a_v[...], w_v[pl.ds(row, size), :], preferred_element_type=f32)
            at = slice(i * WIDE, (i + 1) * WIDE)
            if part == 0:
                yacc[g, :, at] = y
                continue
            y = yacc[g, :, at] + y
            for j in range(WIDE // LANES):
                block = i * (WIDE // LANES) + j
                ysend[g, block // y_blocks, y_rows_at(block % y_blocks), :] = y[:, j * LANES:(j + 1) * LANES]

    def half(h):
        return pl.ds(pl.multiple_of(h * y_cols, LANES), y_cols)

    combine(0)

    with jax.named_scope('wo_wait'):
        for g in range(chips):
            wait_group(0, g)
    for g in range(chips):
        y_rows(0, g)
    combine(1)
    last = chips - 1
    for g in range(chips):
        with jax.named_scope('wo_wait'):
            wait_group(1, g)
        y_rows(1, g)
        if g < last:
            for k in range(2):
                send(ysend.at[g, k], ybuf.at[me], y_ssem, y_rsem, 2 * group_chip[g] + k)
    send(ysend.at[last, 1 - core], ybuf.at[me], y_ssem, y_rsem, peers[-1])
    ybuf[me] = ysend[last, core]
    with jax.named_scope('y_recv'):
        wait_bytes(ybuf.at[pl.ds(0, n_dev - 1)], y_rsem)
    y_sum = ybuf[0]
    for d in range(1, n_dev):
        y_sum = y_sum + ybuf[d]
    for j in range(y_blocks):
        at = pl.ds(pl.multiple_of(me * y_cols + j * LANES, LANES), LANES)
        y_v[:, at] = (x_v[:, at].astype(f32) + y_sum[y_rows_at(j), :]).astype(bf16)
    send_all(y_v.at[:, half(me)], g_ssem, g_rsem)
    with jax.named_scope('g_recv'):
        wait_bytes(y_v.at[:, pl.ds(0, (n_dev - 1) * y_cols)], g_rsem)
    y_out[...] = y_v[...]

    for part in range(2):
        q_buf, _, _, obuf, _, _, mlbuf = part_refs[part][:7]
        n_heads = part_heads[part]
        wait_bytes(q_buf.at[pl.ds(0, (n_dev - 1) * n_heads)], q_ssem.at[part])
        wait_bytes(obuf.at[pl.ds(0, n_dev - 1)], o_ssem.at[part])
        wait_bytes(mlbuf.at[pl.ds(0, n_dev - 1)], ml_ssem.at[part])

    @pl.when(me < 2)
    def _():
        for p in peers:
            wait_bytes(kvbuf.at[0], kv_ssem)

    wait_bytes(ybuf.at[pl.ds(0, n_dev - 1)], y_ssem)
    wait_bytes(y_v.at[:, pl.ds(0, (n_dev - 1) * y_cols)], g_ssem)


def store_kernel(*refs):
    sems, n_out = refs[-1], len(refs) // 2
    copies = [pltpu.make_async_copy(refs[i], refs[n_out + i], sems.at[i]) for i in range(n_out)]
    for c in copies:
        c.start()
    for c in copies:
        c.wait()


def solution(mesh):
    n_dev = mesh.shape["model"]

    def local_step(x, w_q, w_k, w_v, w_o, k_cache, v_cache, lengths):
        rows, _, t_local, head_dim = k_cache.shape
        depth = x.shape[1]
        own_heads = w_q.shape[1] // head_dim
        y_cols = w_o.shape[1] // n_dev
        chips = n_dev // 2
        f32, bf16 = jnp.float32, jnp.bfloat16

        def part_scratch(n_heads, batch):
            return [
                pltpu.VMEM((n_dev * n_heads, rows, head_dim), f32),
                pltpu.VMEM((rows, n_dev * n_heads, head_dim), f32),
                pltpu.VMEM((rows // batch, n_dev, batch * n_heads, head_dim), f32),
                pltpu.VMEM((n_dev, rows // batch, batch * n_heads, head_dim), f32),
                pltpu.VMEM((2, n_dev * n_heads, LANES), f32),
                pltpu.VMEM((n_dev, 2, n_heads, LANES), f32),
                pltpu.VMEM((n_dev, 2, n_heads, LANES), f32),
                pltpu.VMEM((rows, n_heads * head_dim), bf16),
                pltpu.VMEM((rows, n_heads, head_dim), f32),
            ]

        hbm = pl.BlockSpec(memory_space=pl.ANY)
        dma = pltpu.SemaphoreType.DMA
        vm = pl.BlockSpec(memory_space=pltpu.VMEM)
        y, k_new, v_new = pl.pallas_call(
            functools.partial(kernel, n_dev),
            out_shape=(pltpu.VMEM((rows, depth), bf16),
                       pltpu.VMEM((rows, head_dim), bf16),
                       pltpu.VMEM((rows, head_dim), bf16)),
            in_specs=[hbm] * 8,
            out_specs=(vm, vm, vm),
            scratch_shapes=[
                pltpu.SMEM((rows,), jnp.int32),
                pltpu.VMEM((rows, depth), bf16),
                pltpu.VMEM((w_o.shape[0] * w_o.shape[1] // WIDE, WIDE), bf16),
                pltpu.VMEM((depth, head_dim), bf16),
                pltpu.VMEM((rows, t_local, head_dim), bf16),
                pltpu.VMEM((rows, t_local, head_dim), bf16),
                pltpu.VMEM((rows, head_dim, t_local), bf16),
                pltpu.VMEM((2, rows, head_dim), f32),
                pltpu.VMEM((3, FIRST * n_dev, t_local), f32),
                pltpu.VMEM((chips, rows, 2 * y_cols), f32),
                pltpu.VMEM((chips, 2, rows * y_cols // LANES, LANES), f32),
                pltpu.VMEM((n_dev, rows * y_cols // LANES, LANES), f32),
                pltpu.VMEM((rows, depth), bf16),
                *part_scratch(FIRST, SENDS[0]), *part_scratch(own_heads - FIRST, SENDS[1]),
                dma, dma, dma((RING,)), dma, dma((rows,)), dma((rows,)), dma((2, chips)),
                dma, dma((2,)),
            ] + [dma] * 4 + [dma((2,))] * 6,
            compiler_params=pltpu.CompilerParams(
                collective_id=0, has_side_effects=True, vmem_limit_bytes=63000000),
        )(x, w_q, w_k, w_v, w_o, k_cache, v_cache, lengths)
        outs = (y, k_new, v_new)
        return pl.pallas_call(
            store_kernel,
            out_shape=tuple(jax.ShapeDtypeStruct(o.shape, o.dtype) for o in outs),
            in_specs=[hbm] * 3,
            out_specs=(hbm,) * 3,
            scratch_shapes=[dma((len(outs),))],
            compiler_params=pltpu.CompilerParams(vmem_limit_bytes=1 << 20),
        )(*outs)

    row_spec = P("replica", None)
    cache_spec = P("replica", None, "model", None)
    return jax.shard_map(
        local_step, mesh=mesh,
        in_specs=(row_spec, P(None, "model"), P(), P(), P("model", None), cache_spec, cache_spec, P("replica")),
        out_specs=(row_spec, row_spec, row_spec), check_vma=False)
```

```python
import functools
import math

import jax
import jax.numpy as jnp
from jax import lax
from jax.experimental import pallas as pl
from jax.experimental.pallas import tpu as pltpu
from jax.sharding import PartitionSpec as P

RING = 4
LANES = 128
WIDE = 256
FIRST = 4
CHUNK = 256
PAIR = 2
MESH = pl.DeviceIdType.MESH


def kernel(n_dev, x_hbm, wq_hbm, wk_hbm, wv_hbm, wo_hbm, kc_hbm, vc_hbm, len_hbm,
           y_out, k_out, v_out,
           len_s, x_v, w_v, wkv_v, k_v, v_v, kt_v, kvbuf, s_buf, p_buf, yacc, ysend, ybuf, y_v, *rest):
    part_refs, sems = (rest[:9], rest[9:18]), rest[18:]
    (len_sem, x_sem, wq_sem, wkv_sem, k_sem, v_sem, wo_sem,
     kv_ssem, kv_rsem, y_ssem, y_rsem, g_ssem, g_rsem, q_ssem, q_rsem, o_ssem, o_rsem, ml_ssem, ml_rsem) = sems
    rows, depth = x_hbm.shape
    head_dim = wk_hbm.shape[1]
    own_heads = wq_hbm.shape[1] // head_dim
    t_local = kc_hbm.shape[2]
    y_cols = wo_hbm.shape[1] // n_dev
    o_rows = wo_hbm.shape[0]
    chips = n_dev // 2
    pieces = 2 * y_cols // WIDE
    ring_base = w_v.shape[0] - RING * depth
    part_heads = (FIRST, own_heads - FIRST)
    part_row0 = (0, FIRST * head_dim)
    me = lax.axis_index("model")
    chip, core = lax.div(me, 2), lax.rem(me, 2)
    factor = head_dim ** -0.5 * math.log2(math.e)
    f32, bf16 = jnp.float32, jnp.bfloat16

    def chip_at(delta):
        c_x = lax.rem(lax.rem(chip, 2) + delta % 2, 2)
        c_y = lax.rem(lax.div(chip, 2) + delta // 2, 2)
        return c_y * 2 + c_x

    def peer(d_chip, d_core):
        return chip_at(d_chip) * 2 + lax.rem(core + d_core, 2)

    peers = [peer(dc, dk) for dc, dk in ((3, 0), (3, 1), (1, 0), (2, 0), (1, 1), (2, 1), (0, 1))]
    group_chip = [chip_at(d) for d in (3, 1, 2, 0)]

    def cols(i, width):
        return pl.ds(pl.multiple_of(i * width, LANES), width)

    def wq_slot(h):
        return pl.ds(pl.multiple_of(ring_base + lax.rem(h, RING) * depth, 256), depth)

    def wq_copy(h):
        return pltpu.make_async_copy(
            wq_hbm.at[:, cols(h, head_dim)], w_v.at[wq_slot(h), :], wq_sem.at[lax.rem(h, RING)])

    def wo_copy(part, g, i):
        size = part_heads[part] * head_dim
        return pltpu.make_async_copy(
            wo_hbm.at[pl.ds(part_row0[part], size), cols(group_chip[g] * pieces + i, WIDE)],
            w_v.at[pl.ds((g * pieces + i) * o_rows + part_row0[part], size), :], wo_sem.at[part, g])

    def wait_bytes(ref, sem):
        pltpu.make_async_copy(ref, ref, sem).wait()

    def wait_group(part, g):
        wait_bytes(w_v.at[pl.ds(0, pieces * part_heads[part] * head_dim), :], wo_sem.at[part, g])

    def send(src, dst, ssem, rsem, p):
        pltpu.make_async_remote_copy(
            src_ref=src, dst_ref=dst, send_sem=ssem, recv_sem=rsem,
            device_id={"model": p}, device_id_type=MESH).start()

    def send_all(ref, ssem, rsem):
        for p in peers:
            send(ref, ref, ssem, rsem, p)

    x_copy = pltpu.make_async_copy(x_hbm, x_v, x_sem)
    len_copy = pltpu.make_async_copy(len_hbm, len_s, len_sem)
    wk_copy = pltpu.make_async_copy(wk_hbm, wkv_v, wkv_sem)
    wv_copy = pltpu.make_async_copy(wv_hbm, wkv_v, wkv_sem)

    def k_copy(b):
        return pltpu.make_async_copy(kc_hbm.at[b, 0], k_v.at[b], k_sem.at[b])

    def v_copy(b):
        return pltpu.make_async_copy(vc_hbm.at[b, 0], v_v.at[b], v_sem.at[b])

    x_copy.start()
    wq_copy(0).start()
    barrier = pltpu.get_barrier_semaphore()
    for p in peers:
        pl.semaphore_signal(barrier, inc=1, device_id={"model": p}, device_id_type=MESH)
    for h in range(1, RING):
        wq_copy(h).start()
    len_copy.start()
    with jax.named_scope('x_wait'):
        x_copy.wait()

    def q_loop(part):
        q_buf, n_heads = part_refs[part][0], part_heads[part]
        h0 = 0 if part == 0 else FIRST

        def q_step(h, c):
            with jax.named_scope('q_wait'):
                wq_copy(h).wait()
            q = jnp.dot(x_v[...], w_v[wq_slot(h), :], preferred_element_type=f32)
            block = me * n_heads + h - h0
            q_buf[block] = q.astype(bf16).astype(f32)
            if part == 0:
                @pl.when(h == 0)
                def _():
                    with jax.named_scope('barrier'):
                        pl.semaphore_wait(barrier, n_dev - 1)

            send_all(q_buf.at[block], q_ssem.at[part], q_rsem.at[part])
            if h0 < own_heads - RING:
                @pl.when(h < own_heads - RING)
                def _():
                    wq_copy(h + RING).start()

            if part == 1:
                @pl.when((h == h0) & (me == 0))
                def _():
                    wk_copy.start()

                @pl.when((h == h0) & (me == 1))
                def _():
                    wv_copy.start()

                @pl.when(h == h0 + 1)
                def _():
                    def start_kv(b, c):
                        k_copy(b).start()
                        v_copy(b).start()
                        return c
                    lax.fori_loop(0, rows, start_kv, 0)
            return c

        lax.fori_loop(h0, h0 + n_heads, q_step, 0)

    q_loop(0)
    q_loop(1)
    for part in range(2):
        for g in range(chips):
            for i in range(pieces):
                wo_copy(part, g, i).start()

    positions = me * t_local + lax.broadcasted_iota(jnp.int32, (1, t_local), 1)

    def part_rows(part, b):
        n = (b % PAIR) * part_heads[part]
        return slice(n, n + part_heads[part])

    chunks = [slice(c, c + CHUNK) for c in range(0, t_local, CHUNK)]
    ml = [jnp.zeros((n * n_dev, LANES), f32) for n in part_heads]

    def wait_q(part):
        with jax.named_scope('q_recv'):
            wait_bytes(part_refs[part][0].at[pl.ds(0, (n_dev - 1) * part_heads[part])], q_rsem.at[part])

    def wait_kv(b):
        with jax.named_scope('kv_wait'):
            for c in range(b, b + PAIR):
                k_copy(c).wait()
                v_copy(c).wait()

    def scores(b, parts, transposed):
        q_b = jnp.concatenate([part_refs[p][0][:, b, :] for p in parts], axis=0).astype(bf16)
        if transposed:
            s = jnp.dot(q_b, kt_v[b], preferred_element_type=f32)
        else:
            s = lax.dot_general(q_b, k_v[b], (((1,), (1,)), ((), ())), preferred_element_type=f32)
        s_buf[b % 3, :q_b.shape[0]] = s

    def attend(b, parts):
        n_rows = sum(part_heads[p] for p in parts) * n_dev

        def masked(at):
            return jnp.where(positions[:, at] < len_s[b], s_buf[b % 3, :n_rows, at], -jnp.inf)

        m = functools.reduce(jnp.maximum, [masked(at) for at in chunks])
        m = jnp.max(m, axis=1, keepdims=True)
        m_safe = jnp.where(m == -jnp.inf, 0.0, m)
        l = jnp.zeros((n_rows, CHUNK), f32)
        for at in chunks:
            p = jnp.exp2((masked(at) - m_safe) * factor)
            l = l + p
            hi = p.astype(bf16)
            p_buf[b % 2, :n_rows, at] = hi
            p_buf[b % 2, n_rows:2 * n_rows, at] = (p - hi.astype(f32)).astype(bf16)
        l = jnp.sum(l, axis=1, keepdims=True)
        o2 = jnp.dot(p_buf[b % 2, :2 * n_rows], v_v[b], preferred_element_type=f32)
        o = o2[:n_rows] + o2[n_rows:]
        row = 0
        for part in parts:
            n_heads = part_heads[part]
            here = slice(row, row + n_heads * n_dev)
            row += n_heads * n_dev
            lane = lax.broadcasted_iota(jnp.int32, (n_heads * n_dev, LANES), 1)
            ml[part] = jnp.where(lane == b, m[here], ml[part])
            ml[part] = jnp.where(lane == b + LANES // 2, l[here], ml[part])
            _, o_flat, osend = part_refs[part][:3]
            o_flat[b] = o[here]
            for d in range(n_dev):
                osend[b // PAIR, d, part_rows(part, b), :] = o_flat[b, d * n_heads:(d + 1) * n_heads, :]

    def send_ml(part):
        mlflat, mlsend, mlbuf = part_refs[part][4:7]
        n_heads = part_heads[part]
        mlflat[...] = ml[part]
        for d in range(n_dev):
            mlsend[d] = mlflat[d * n_heads:(d + 1) * n_heads, :]
        mlbuf[me] = mlsend[me]
        for d in peers:
            send(mlsend.at[d], mlbuf.at[me], ml_ssem.at[part], ml_rsem.at[part], d)

    def send_o(part, n):
        _, _, osend, obuf = part_refs[part][:4]
        obuf[me, n] = osend[n, me]
        for d in peers:
            send(osend.at[n, d], obuf.at[me, n], o_ssem.at[part], o_rsem.at[part], d)

    tail = rows - PAIR

    def attention_first():
        wait_q(0)
        len_copy.wait()
        for b in range(0, tail, PAIR):
            wait_kv(b)
            for c in range(b, b + PAIR):
                kt_v[c] = k_v[c].T
                scores(c, (0,), False)
            for c in range(b, b + PAIR):
                attend(c, (0,))
            send_o(0, b // PAIR)

    def attention_second():
        wait_q(1)
        wait_kv(tail)
        for c in range(tail, rows):
            scores(c, (0, 1), False)
        for c in range(tail, rows):
            attend(c, (0, 1))
        send_ml(0)
        send_o(0, tail // PAIR)
        send_o(1, tail // PAIR)
        for c in range(PAIR):
            scores(c, (1,), True)
        for b in range(tail):
            if b + PAIR < tail:
                scores(b + PAIR, (1,), True)
            attend(b, (1,))
            if (b + 1) % PAIR == 0:
                if b + 1 == tail:
                    send_ml(1)
                send_o(1, b // PAIR)

    @pl.when(me < 2)
    def _():
        with jax.named_scope('wkv_wait'):
            wk_copy.wait()
        kv = jnp.dot(x_v[...], wkv_v[...], preferred_element_type=f32)
        kvbuf[me] = kv.astype(bf16).astype(f32)
        for p in peers:
            send(kvbuf.at[me], kvbuf.at[me], kv_ssem, kv_rsem.at[me], p)

    attention_first()
    attention_second()

    for i in range(2):
        @pl.when(me != i)
        def _():
            with jax.named_scope('kv_recv'):
                wait_bytes(kvbuf.at[i], kv_rsem.at[i])
    k_new, v_new = kvbuf[0], kvbuf[1]
    k_out[...] = k_new.astype(bf16)
    v_out[...] = v_new.astype(bf16)

    def combine(part):
        q_buf, _, _, obuf, _, _, mlbuf, a_v, astage = part_refs[part]
        n_heads = part_heads[part]
        lane = lax.broadcasted_iota(jnp.int32, (n_heads, LANES), 1)
        with jax.named_scope('ml_recv'):
            wait_bytes(mlbuf.at[pl.ds(0, n_dev - 1)], ml_rsem.at[part])
        s_new = jnp.zeros((n_heads, LANES), f32)
        for b in range(rows):
            q_own = q_buf[pl.ds(me * n_heads, n_heads), b, :]
            s_new = jnp.where(lane == b, jnp.sum(q_own * k_new[b:b + 1, :], axis=1, keepdims=True), s_new)
        top = s_new
        for d in range(n_dev):
            top = jnp.maximum(top, mlbuf[d])
        w_new = jnp.exp2((s_new - top) * factor)
        w = [jnp.exp2((mlbuf[d] - top) * factor) for d in range(n_dev)]
        total = w_new
        for d in range(n_dev):
            total = total + w[d] * pltpu.roll(mlbuf[d], LANES // 2, 1)
        inv = 1.0 / total
        w_new = w_new * inv
        w = [w_d * inv for w_d in w]
        with jax.named_scope('o_recv'):
            wait_bytes(obuf.at[pl.ds(0, n_dev - 1)], o_rsem.at[part])
        for b in range(rows):
            acc = w_new[:, b:b + 1] * v_new[b:b + 1, :]
            for d in range(n_dev):
                acc = acc + w[d][:, b:b + 1] * obuf[d, b // PAIR, part_rows(part, b), :]
            astage[b] = acc
        for h in range(n_heads):
            a_v[:, h * head_dim:(h + 1) * head_dim] = astage[:, h, :].astype(bf16)

    y_blocks = y_cols // LANES

    def y_rows_at(block):
        return slice(block * rows, (block + 1) * rows)

    def y_dot(g, i, parts):
        a = jnp.concatenate([part_refs[p][7][...] for p in parts], axis=1)
        row = (g * pieces + i) * o_rows + part_row0[parts[0]]
        return jnp.dot(a, w_v[pl.ds(row, a.shape[1]), :], preferred_element_type=f32)

    def y_store(g, i, y):
        for j in range(WIDE // LANES):
            block = i * (WIDE // LANES) + j
            ysend[g, block // y_blocks, y_rows_at(block % y_blocks), :] = y[:, j * LANES:(j + 1) * LANES]

    def piece_cols(i):
        return slice(i * WIDE, (i + 1) * WIDE)

    def half(h):
        return pl.ds(pl.multiple_of(h * y_cols, LANES), y_cols)

    combine(0)

    last = chips - 1
    with jax.named_scope('wo_wait'):
        for g in range(last):
            wait_group(0, g)
    for g in range(last):
        for i in range(pieces):
            yacc[g, :, piece_cols(i)] = y_dot(g, i, (0,))
    combine(1)
    for g in range(last):
        with jax.named_scope('wo_wait'):
            wait_group(1, g)
        for i in range(pieces):
            y_store(g, i, yacc[g, :, piece_cols(i)] + y_dot(g, i, (1,)))
        for k in range(2):
            send(ysend.at[g, k], ybuf.at[me], y_ssem, y_rsem, 2 * group_chip[g] + k)
    with jax.named_scope('wo_wait'):
        wait_group(0, last)
        wait_group(1, last)
    for i in range(pieces):
        y_store(last, i, y_dot(last, i, (0, 1)))
    send(ysend.at[last, 1 - core], ybuf.at[me], y_ssem, y_rsem, peers[-1])
    ybuf[me] = ysend[last, core]
    with jax.named_scope('y_recv'):
        wait_bytes(ybuf.at[pl.ds(0, n_dev - 1)], y_rsem)
    y_sum = ybuf[0]
    for d in range(1, n_dev):
        y_sum = y_sum + ybuf[d]
    for j in range(y_blocks):
        at = pl.ds(pl.multiple_of(me * y_cols + j * LANES, LANES), LANES)
        y_v[:, at] = (x_v[:, at].astype(f32) + y_sum[y_rows_at(j), :]).astype(bf16)
    send_all(y_v.at[:, half(me)], g_ssem, g_rsem)
    for part in range(2):
        q_buf, _, _, obuf, _, _, mlbuf = part_refs[part][:7]
        n_heads = part_heads[part]
        wait_bytes(q_buf.at[pl.ds(0, (n_dev - 1) * n_heads)], q_ssem.at[part])
        wait_bytes(obuf.at[pl.ds(0, n_dev - 1)], o_ssem.at[part])
        wait_bytes(mlbuf.at[pl.ds(0, n_dev - 1)], ml_ssem.at[part])

    @pl.when(me < 2)
    def _():
        for p in peers:
            wait_bytes(kvbuf.at[0], kv_ssem)

    wait_bytes(ybuf.at[pl.ds(0, n_dev - 1)], y_ssem)
    wait_bytes(y_v.at[:, pl.ds(0, (n_dev - 1) * y_cols)], g_ssem)
    with jax.named_scope('g_recv'):
        wait_bytes(y_v.at[:, pl.ds(0, (n_dev - 1) * y_cols)], g_rsem)
    y_out[...] = y_v[...]


def store_kernel(*refs):
    sems, n_out = refs[-1], len(refs) // 2
    copies = [pltpu.make_async_copy(refs[i], refs[n_out + i], sems.at[i]) for i in range(n_out)]
    for c in copies:
        c.start()
    for c in copies:
        c.wait()


def solution(mesh):
    n_dev = mesh.shape["model"]

    def local_step(x, w_q, w_k, w_v, w_o, k_cache, v_cache, lengths):
        rows, _, t_local, head_dim = k_cache.shape
        depth = x.shape[1]
        own_heads = w_q.shape[1] // head_dim
        y_cols = w_o.shape[1] // n_dev
        chips = n_dev // 2
        f32, bf16 = jnp.float32, jnp.bfloat16

        def part_scratch(n_heads):
            return [
                pltpu.VMEM((n_dev * n_heads, rows, head_dim), f32),
                pltpu.VMEM((rows, n_dev * n_heads, head_dim), f32),
                pltpu.VMEM((rows // PAIR, n_dev, PAIR * n_heads, head_dim), f32),
                pltpu.VMEM((n_dev, rows // PAIR, PAIR * n_heads, head_dim), f32),
                pltpu.VMEM((n_dev * n_heads, LANES), f32),
                pltpu.VMEM((n_dev, n_heads, LANES), f32),
                pltpu.VMEM((n_dev, n_heads, LANES), f32),
                pltpu.VMEM((rows, n_heads * head_dim), bf16),
                pltpu.VMEM((rows, n_heads, head_dim), f32),
            ]

        hbm = pl.BlockSpec(memory_space=pl.ANY)
        dma = pltpu.SemaphoreType.DMA
        vm = pl.BlockSpec(memory_space=pltpu.VMEM)
        y, k_new, v_new = pl.pallas_call(
            functools.partial(kernel, n_dev),
            out_shape=(pltpu.VMEM((rows, depth), bf16),
                       pltpu.VMEM((rows, head_dim), bf16),
                       pltpu.VMEM((rows, head_dim), bf16)),
            in_specs=[hbm] * 8,
            out_specs=(vm, vm, vm),
            scratch_shapes=[
                pltpu.SMEM((rows,), jnp.int32),
                pltpu.VMEM((rows, depth), bf16),
                pltpu.VMEM((w_o.shape[0] * w_o.shape[1] // WIDE, WIDE), bf16),
                pltpu.VMEM((depth, head_dim), bf16),
                pltpu.VMEM((rows, t_local, head_dim), bf16),
                pltpu.VMEM((rows, t_local, head_dim), bf16),
                pltpu.VMEM((rows, head_dim, t_local), bf16),
                pltpu.VMEM((2, rows, head_dim), f32),
                pltpu.VMEM((3, own_heads * n_dev, t_local), f32),
                pltpu.VMEM((2, 2 * own_heads * n_dev, t_local), bf16),
                pltpu.VMEM((chips - 1, rows, 2 * y_cols), f32),
                pltpu.VMEM((chips, 2, rows * y_cols // LANES, LANES), f32),
                pltpu.VMEM((n_dev, rows * y_cols // LANES, LANES), f32),
                pltpu.VMEM((rows, depth), bf16),
                *part_scratch(FIRST), *part_scratch(own_heads - FIRST),
                dma, dma, dma((RING,)), dma, dma((rows,)), dma((rows,)), dma((2, chips)),
                dma, dma((2,)),
            ] + [dma] * 4 + [dma((2,))] * 6,
            compiler_params=pltpu.CompilerParams(
                collective_id=0, has_side_effects=True, vmem_limit_bytes=63000000),
        )(x, w_q, w_k, w_v, w_o, k_cache, v_cache, lengths)
        outs = (y, k_new, v_new)
        return pl.pallas_call(
            store_kernel,
            out_shape=tuple(jax.ShapeDtypeStruct(o.shape, o.dtype) for o in outs),
            in_specs=[hbm] * 3,
            out_specs=(hbm,) * 3,
            scratch_shapes=[dma((len(outs),))],
            compiler_params=pltpu.CompilerParams(vmem_limit_bytes=1 << 20),
        )(*outs)

    row_spec = P("replica", None)
    cache_spec = P("replica", None, "model", None)
    return jax.shard_map(
        local_step, mesh=mesh,
        in_specs=(row_spec, P(None, "model"), P(), P(), P("model", None), cache_spec, cache_spec, P("replica")),
        out_specs=(row_spec, row_spec, row_spec), check_vma=False)
```
